32 devices in a mesh: energy: 4 (over z), block: 4 (over y, x), role: 2 (over core).
Axes of the slice: x: 2, y: 2, z: 4, core: 2. Of those that a mesh axis runs over, the one named last changes fastest.
Arguments:
- sigma_in: float32 [2, 8, 4, 128, 128], P(None, ('energy', 'role'), 'block'), may hold values from -0.009 to 0.009
- hamiltonian: float32 [4, 128, 128], P('block'), may hold values from -0.5 to 0.5
- coupling: float32 [4, 128, 128], P('block'), may hold values from -0.25 to 0.25
- coulomb: float32 [4, 16384], P('block', ('energy', 'role')), may hold values from 0.2 to 1
- pattern: int32 [2, 4, 4, 4], P(None, 'block'), may hold values 0 or 1
- offsets: int32 [16], replicated, may hold values from 0 to 3
Outputs:
- green: float32 [2, 8, 4, 128, 128], P(None, ('energy', 'role'), 'block')
- sigma_out: float32 [2, 8, 4, 128, 128], P(None, ('energy', 'role'), 'block')
The draws below stay inside these ranges and needn't reach their ends.
All inputs are finite; a program needn't handle non-finite values. No bound on the sum of `pattern` on one device may be relied on, other than what follows from the above.
Results may differ from the reference program's by a relative error of at most 0.0003.
Values sent between devices are 32-bit elements; how exact they have to be, the bound alone decides.
No kernel may reach another device: no remote copies, remote signals or barrier semaphores. Data moves between devices by JAX's collectives and lax.ppermute only.
A program may use at most 64 MiB of HBM per device.

```python
import jax
import jax.numpy as jnp
from jax import lax

M = 128
TILE = 32
NW = 16
NB = 4
NE = 8
TL = 4


def place_ends(values, stream_key, smallest, top_value):
    dims = values.shape
    index_at = [jax.random.randint(jax.random.fold_in(stream_key, axis), (), 0, dims[axis]) for axis in range(len(dims))]
    values = values.at[tuple(index_at)].set(smallest)
    longest = dims.index(max(dims))
    index_at[longest] = (index_at[longest] + 1) % dims[longest]
    return values.at[tuple(index_at)].set(top_value)


def steps_of(rng, dims, split, low, largest):
    level, own = 1.0, jax.random.fold_in(rng, 6)
    for position, parts in split:
        heights = jnp.exp(jax.random.uniform(jax.random.fold_in(own, position), (parts,), jnp.float32, low / len(split), largest / len(split)))
        level = level * jnp.repeat(heights, dims[position] // parts).reshape([-1 if axis == position else 1 for axis in range(len(dims))])
    return level


def bell_draw(own_key, extent, scale, limit, shards=(), held_as=jnp.bfloat16):
    values = scale * jax.random.normal(own_key, extent, jnp.float32)
    if shards:
        values = values * steps_of(own_key, extent, shards, -0.22, 0.18)
    return jnp.clip(values, -limit, limit).astype(held_as)


def setup_inputs(seed: int = 0) -> dict:
    seeds = jax.random.split(jax.random.key(seed), 7)
    sigma_in = bell_draw(seeds[0], (2, NE, NB, M, M), 0.0015, 0.009, ((1, 8), (2, 4)), jnp.float32)
    hamiltonian = bell_draw(seeds[1], (NB, M, M), M ** -0.5, 0.5, ((0, 4),), jnp.float32)
    coupling = bell_draw(seeds[2], (NB, M, M), (4 * M) ** -0.5, 0.25, ((0, 4),), jnp.float32)
    coulomb = jnp.clip(0.2 + 0.8 * jax.random.uniform(seeds[3], (NB, M * M), jnp.float32) ** steps_of(seeds[3], (NB, M * M), ((0, 4), (1, 8)), -0.2, 0.2), 0.2, 1.0)
    pattern = place_ends((jax.random.randint(seeds[4], (2, NB, TL, TL), 0, 4) < 3).astype(jnp.int32), jax.random.fold_in(seeds[4], 1), 0, 1)
    offsets = place_ends(jax.random.randint(seeds[5], (NW,), 0, NE // 2), jax.random.fold_in(seeds[5], 1), 0, (NE // 2) - 1).astype(jnp.int32)
    return {"sigma_in": sigma_in, "hamiltonian": hamiltonian, "coupling": coupling, "coulomb": coulomb, "pattern": pattern, "offsets": offsets}


ETA = 0.1
CONTACT = 0.5
HIGH = lax.Precision.HIGHEST

def real_product(left_part, right_part):
    return jnp.einsum('...ij,...jk->...ik', left_part.astype(jnp.float32), right_part.astype(jnp.float32), precision=HIGH, preferred_element_type=jnp.float32)

def complex_dot(first, second):
    rr = real_product(first[0], second[0]) - real_product(first[1], second[1])
    ri = real_product(first[0], second[1]) + real_product(first[1], second[0])
    return jnp.stack([rr, ri])

def real_left(matrix, value):
    return jnp.einsum('ij,...jk->...ik', matrix.astype(jnp.float32), value.astype(jnp.float32), precision=HIGH, preferred_element_type=jnp.float32)

def real_right(value, matrix):
    return jnp.einsum('...ij,jk->...ik', value.astype(jnp.float32), matrix.astype(jnp.float32), precision=HIGH, preferred_element_type=jnp.float32)

def expand(tiles):
    count = tiles.shape[-1]
    lead = tiles.shape[:-2]
    big = jnp.broadcast_to(tiles[..., :, None, :, None], lead + (count, TILE, count, TILE))
    return big.reshape(lead + (count * TILE, count * TILE)).astype(jnp.float32)

def symmetric(block):
    return 0.5 * (block + jnp.swapaxes(block, -1, -2))

def system_matrix(energy, onsite_block, sigma_block, identity):
    real_part = energy[:, None, None] * identity - onsite_block - sigma_block[0]
    imag_part = ETA * identity - sigma_block[1]
    return jnp.stack([real_part, imag_part])

def contact(system, coupling_block, ends):
    square_coupling = jnp.dot(coupling_block.T.astype(jnp.float32), coupling_block.astype(jnp.float32), precision=HIGH, preferred_element_type=jnp.float32)
    return jnp.stack([system[0], system[1] + ends * CONTACT * square_coupling])

def invert(system):
    width = system.shape[-1]
    a_part = system[0]
    b_part = system[1]
    a_trans = jnp.swapaxes(a_part, -1, -2)
    b_trans = jnp.swapaxes(b_part, -1, -2)
    p_part = real_product(a_trans, a_part) + real_product(b_trans, b_part)
    q_part = real_product(a_trans, b_part) - real_product(b_trans, a_part)
    upper_rows = jnp.concatenate([p_part, -q_part], axis=-1)
    lower_rows = jnp.concatenate([q_part, p_part], axis=-1)
    normal = jnp.concatenate([upper_rows, lower_rows], axis=-2)
    factor = jnp.linalg.cholesky(normal)
    stacked = jnp.concatenate([a_trans, -b_trans], axis=-2)
    middle = jax.scipy.linalg.solve_triangular(factor, stacked, lower=True)
    solved = jax.scipy.linalg.solve_triangular(factor, middle, lower=True, trans=1)
    return jnp.stack([solved[..., :width, :], solved[..., width:, :]])

def project(coupling_block, left_green):
    return real_right(real_left(coupling_block.T, left_green), coupling_block)

def backstep(left_green, coupling_block, right_full):
    first = real_right(left_green, coupling_block)
    second = complex_dot(first, right_full)
    third = real_right(second, coupling_block.T)
    return left_green + complex_dot(third, left_green)

def screen(values, offsets):
    energies = values.shape[1]
    factor = 6.0 / energies / (2.0 * 3.141592653589793)
    widths = ((0, 0), (energies, 0)) + ((0, 0),) * (values.ndim - 2)
    padded = jnp.pad(values, widths)

    def one_offset(offset_index, total):
        start = (energies - offsets[offset_index]).astype(jnp.int32)
        moved = lax.dynamic_slice_in_dim(padded, start, energies, 1)
        pol_real = factor * jnp.sum(values[0] * moved[0] - values[1] * moved[1], axis=0)
        pol_imag = factor * jnp.sum(values[0] * moved[1] + values[1] * moved[0], axis=0)
        self_real = moved[0] * pol_real - moved[1] * pol_imag
        self_imag = moved[0] * pol_imag + moved[1] * pol_real
        return total + jnp.stack([self_real, self_imag])
    summed = lax.fori_loop(0, offsets.shape[0], one_offset, jnp.zeros_like(values))
    return summed / offsets.shape[0]

def reference(sigma_in, hamiltonian, coupling, coulomb, pattern, offsets):
    identity = jnp.eye(M, dtype=jnp.float32)
    masks = expand(pattern)
    energy = -3.0 + 6.0 * jnp.arange(NE).astype(jnp.float32) / NE
    lefts = []
    sent = None
    for block_index in range(NB):
        onsite = symmetric(hamiltonian[block_index] * masks[0, block_index])
        system = system_matrix(energy, onsite, sigma_in[:, :, block_index], identity)
        if block_index == NB - 1:
            system = contact(system, coupling[block_index], 1.0)
        if block_index > 0:
            system = system - sent
        left_green = invert(system)
        lefts.append(left_green)
        if block_index < NB - 1:
            sent = project(coupling[block_index], left_green)
    full = lefts[-1]
    fulls = [full]
    for block_index in range(NB - 2, -1, -1):
        full = backstep(lefts[block_index], coupling[block_index], full)
        fulls.insert(0, full)
    green = jnp.stack(fulls, axis=2)
    outgoing = []
    for block_index in range(NB):
        summed = screen(green[:, :, block_index], offsets)
        effective = coulomb[block_index].reshape(M, M) * masks[1, block_index]
        outgoing.append(summed * (effective * effective))
    return (green, jnp.stack(outgoing, axis=2))
```

```python
import functools

import jax
import jax.numpy as jnp
from jax import lax
from jax.experimental import pallas as pl
from jax.experimental.pallas import tpu as pltpu
from jax.sharding import PartitionSpec as P

ETA = 0.1
CONTACT = 0.5
HIGH = lax.Precision.HIGHEST
F32 = jnp.float32
BF16 = jnp.bfloat16

LOW = 1e-4
STEPS = 8
POLISH = 2
TOL = 1e-6
MAX_SAFE = 300


def step_table(low, steps):
    rows = []
    for _ in range(steps):
        scale = 4.0 / (1.0 + low) ** 2
        rows.append((scale * (1.0 + low), scale))
        low = scale * low
    return rows, 2.0 / (1.0 + low)


def split(value):
    high = value.astype(BF16)
    return high, (value - high.astype(F32)).astype(BF16)


def dot(left, right):
    return jnp.dot(left, right, preferred_element_type=F32)


def dot3(left, right_high, right_low):
    left_high, left_low = split(left)
    return dot(left_high, right_high) + (dot(left_high, right_low) + dot(left_low, right_high))


def embed(wide):
    half = wide.shape[1] // 2
    return jnp.concatenate(
        [wide, jnp.concatenate([-wide[:, half:], wide[:, :half]], axis=1)], axis=0
    )


def embed_split(wide):
    high, low = split(wide)
    return embed(high), embed(low)


def wide_eye(size):
    row = lax.broadcasted_iota(jnp.int32, (size, 2 * size), 0)
    col = lax.broadcasted_iota(jnp.int32, (size, 2 * size), 1)
    return jnp.where(row == col, 1.0, 0.0).astype(F32)


def adjoint(wide):
    half = wide.shape[1] // 2
    return jnp.concatenate([wide[:, :half].T, -wide[:, half:].T], axis=1)


def invert_many(slots, s_ref, x_ref, z_ref, eh_ref, el_ref):
    size = s_ref.shape[1]
    eye = wide_eye(size)
    table, last = step_table(LOW, STEPS)
    alphas = {}
    for slot in slots:
        value = s_ref[slot]
        high, low = embed_split(value)
        eh_ref[slot] = high
        el_ref[slot] = low
        normal = dot3(adjoint(value), high, low)
        magnitude = jnp.abs(normal[:, :size]) + jnp.abs(normal[:, size:])
        bound = jnp.max(jnp.sum(magnitude, axis=1, keepdims=True), axis=0, keepdims=True)
        alpha = 1.0 / bound
        alphas[slot] = alpha
        first = normal * alpha
        z_ref[slot, :size] = first
        z_ref[slot, size:] = eye
    for index in range(STEPS):
        lift, scale = table[index]
        for slot in slots:
            both = z_ref[slot]
            high, low = embed_split(both[:size])
            z_ref[slot] = lift * both - scale * dot3(both, high, low)
    for slot in slots:
        value = s_ref[slot]
        high, low = embed_split(adjoint(value))
        x_ref[slot] = (last * alphas[slot]) * dot3(z_ref[slot, size:], high, low)
    worst = None
    for _ in range(POLISH):
        worst = None
        for slot in slots:
            approx = x_ref[slot]
            rest = eye - dot3(approx, eh_ref[slot], el_ref[slot])
            high, low = embed_split(approx)
            x_ref[slot] = approx + dot3(rest, high, low)
            size_rest = jnp.sum(rest * rest)
            worst = size_rest if worst is None else jnp.maximum(worst, size_rest)

    @pl.when(jnp.logical_not(worst < TOL))
    def _():
        for slot in slots:
            x_ref[slot] = adjoint(s_ref[slot]) * alphas[slot]

        def unfinished(state):
            return jnp.logical_and(state[0] < MAX_SAFE, jnp.logical_not(state[1] < TOL))

        def refine(state):
            worst = None
            for slot in slots:
                approx = x_ref[slot]
                rest = eye - dot3(approx, eh_ref[slot], el_ref[slot])
                high, low = embed_split(approx)
                x_ref[slot] = approx + dot3(rest, high, low)
                size_rest = jnp.sum(rest * rest)
                worst = size_rest if worst is None else jnp.maximum(worst, size_rest)
            return state[0] + 1, worst

        lax.while_loop(unfinished, refine, (jnp.int32(0), jnp.float32(1e30)))


def prepare_kernel(total, last_block, pattern_ref, sigma_ref, ham_ref, coupling_ref, coulomb_ref, out_ref, weight_ref):
    size = ham_ref.shape[-1]
    tiles = pattern_ref.shape[-1]
    tile = size // tiles
    block = lax.axis_index("block")
    place = lax.axis_index("energy") * lax.axis_size("role") + lax.axis_index("role")

    def mask_rows(which, row_tile):
        lane = lax.broadcasted_iota(jnp.int32, (1, size), 1) // tile
        row = jnp.zeros((1, size), F32)
        for column in range(tiles):
            row = jnp.where(lane == column, pattern_ref[which, 0, row_tile, column].astype(F32), row)
        return row

    mask = jnp.concatenate(
        [jnp.broadcast_to(mask_rows(0, row_tile), (tile, size)) for row_tile in range(tiles)], axis=0
    )
    masked = ham_ref[0] * mask
    onsite = 0.5 * (masked + masked.T)
    row = lax.broadcasted_iota(jnp.int32, (size, size), 0)
    col = lax.broadcasted_iota(jnp.int32, (size, size), 1)
    number = jnp.full((size, size), place, jnp.int32).astype(F32)
    energy = -3.0 + 6.0 * number / total
    out_ref[0] = jnp.where(row == col, energy, 0.0) - onsite - sigma_ref[0, 0, 0]
    out_ref[1] = jnp.where(row == col, ETA, 0.0) - sigma_ref[1, 0, 0]
    out_ref[2] = coupling_ref[0]

    @pl.when(block == last_block)
    def _():
        square = jnp.dot(
            coupling_ref[0].T, coupling_ref[0], precision=HIGH, preferred_element_type=F32
        )
        out_ref[1] += CONTACT * square

    rows = coulomb_ref.shape[0]
    for local_row in range(rows):
        tile_row = (place * rows + local_row) // tile
        lane = lax.broadcasted_iota(jnp.int32, (1, size), 1) // tile
        line = jnp.zeros((1, size), F32)
        for column in range(tiles):
            line = jnp.where(lane == column, pattern_ref[1, 0, tile_row, column].astype(F32), line)
        value = coulomb_ref[local_row : local_row + 1] * line
        weight_ref[local_row : local_row + 1] = value * value


def green_kernel(groups, all_ref, out_ref, pieces_ref, s_ref, x_ref, z_ref, eh_ref, el_ref, k_ref):
    size = all_ref.shape[-1]
    own = lax.axis_index("block")
    far = own ^ 2
    low_half = own % 2 == 0
    middle = jnp.where(low_half, 1, 2)
    other = jnp.where(low_half, 3, 0)

    def base(block):
        return jnp.concatenate([all_ref[block, 0], all_ref[block, 1]], axis=1)

    for block in range(3):
        value = all_ref[block, 2]
        k_ref[block] = value
        k_ref[3 + block] = value.T

    def link(source, target):
        return k_ref[jnp.where(target > source, source, 3 + target)]

    s_ref[0] = base(middle)
    s_ref[1] = base(other)
    invert_many((0, 1), s_ref, x_ref, z_ref, eh_ref, el_ref)

    beside = jnp.where(low_half, 2, 1)
    to_other = link(beside, other)
    both = jnp.concatenate([link(own, middle), link(far, middle)], axis=0)
    both_t = jnp.concatenate([link(middle, own), link(middle, far)], axis=1)

    def congruence(left, value, right):
        high, low = split(value)
        first = dot3(left, high, low)
        rows = jnp.concatenate([first[:, :size], first[:, size:]], axis=0)
        high, low = split(right)
        result = dot3(rows, high, low)
        count = left.shape[0]
        return result[:count], result[count:]

    real, imag = congruence(both, x_ref[0], both_t)
    o_real, o_imag = congruence(to_other, x_ref[1], link(other, beside))
    side = jnp.concatenate([o_real, o_imag], axis=1)
    beside_far = beside == far

    def wide(rows, columns):
        return jnp.concatenate([real[rows, columns], imag[rows, columns]], axis=1)

    top, bottom = slice(0, size), slice(size, 2 * size)
    s_ref[0] = base(far) - wide(bottom, bottom) - jnp.where(beside_far, side, 0.0)
    own_part = base(own) - wide(top, top) - jnp.where(beside_far, 0.0, side)
    up = wide(top, bottom)
    down = wide(bottom, top)
    s_ref[1] = own_part
    z_ref[1, :size] = up
    z_ref[1, size:] = down
    invert_many((0,), s_ref, x_ref, z_ref, eh_ref, el_ref)
    high, low = embed_split(x_ref[0])
    first = dot3(z_ref[1, :size], high, low)
    high, low = embed_split(z_ref[1, size:])
    s_ref[0] = s_ref[1] - dot3(first, high, low)
    invert_many((0,), s_ref, x_ref, z_ref, eh_ref, el_ref)
    result = x_ref[0]
    out_ref[0, 0, 0] = result[:, :size]
    out_ref[1, 0, 0] = result[:, size:]
    rows = size // groups
    for group in range(groups):
        part = slice(group * rows, (group + 1) * rows)
        pieces_ref[group, 0] = result[part, :size]
        pieces_ref[group, 1] = result[part, size:]


def screen_kernel(offsets_ref, weight_ref, g_ref, out_ref):
    energies = g_ref.shape[0]
    count = offsets_ref.shape[0]
    factor = 6.0 / energies / (2.0 * 3.141592653589793) / count
    weight = weight_ref[...]

    def uses(offset):
        return lax.fori_loop(
            0, count, lambda i, total: total + jnp.where(offsets_ref[i] == offset, 1, 0), jnp.int32(0)
        )

    if energies <= 16:
        real = [g_ref[n, 0] for n in range(energies)]
        imag = [g_ref[n, 1] for n in range(energies)]
        out_real = [jnp.zeros_like(weight) for _ in range(energies)]
        out_imag = [jnp.zeros_like(weight) for _ in range(energies)]
        hits = [jnp.int32(0) for _ in range(energies)]
        for index in range(count):
            offset = offsets_ref[index]
            for d in range(energies):
                hits[d] = hits[d] + jnp.where(offset == d, 1, 0)
        for d in range(energies):
            scale = weight * (factor * hits[d].astype(F32))
            p_real = jnp.zeros_like(weight)
            p_imag = jnp.zeros_like(weight)
            for n in range(d, energies):
                p_real += real[n] * real[n - d] - imag[n] * imag[n - d]
                p_imag += real[n] * imag[n - d] + imag[n] * real[n - d]
            p_real *= scale
            p_imag *= scale
            for n in range(d, energies):
                out_real[n] += real[n - d] * p_real - imag[n - d] * p_imag
                out_imag[n] += real[n - d] * p_imag + imag[n - d] * p_real
        for n in range(energies):
            out_ref[n, 0] = out_real[n]
            out_ref[n, 1] = out_imag[n]
    else:
        out_ref[...] = jnp.zeros_like(out_ref)

        @pl.loop(0, energies)
        def _(d):
            hits = uses(d)

            @pl.when(hits > 0)
            def _():
                scale = weight * (factor * hits.astype(F32))

                def gather(n, total):
                    a, b, c, e = g_ref[n, 0], g_ref[n, 1], g_ref[n - d, 0], g_ref[n - d, 1]
                    return total[0] + a * c - b * e, total[1] + a * e + b * c

                zero = jnp.zeros_like(weight)
                p_real, p_imag = lax.fori_loop(d, energies, gather, (zero, zero))
                p_real, p_imag = p_real * scale, p_imag * scale

                @pl.loop(d, energies)
                def _(n):
                    a, b = g_ref[n - d, 0], g_ref[n - d, 1]
                    out_ref[n, 0] += a * p_real - b * p_imag
                    out_ref[n, 1] += a * p_imag + b * p_real


VM = pl.BlockSpec(memory_space=pltpu.VMEM)
SM = pl.BlockSpec(memory_space=pltpu.SMEM)


def body(sigma_in, hamiltonian, coupling, coulomb, pattern, offsets):
    size = hamiltonian.shape[-1]
    blocks = lax.axis_size("block")
    groups = lax.axis_size("energy") * lax.axis_size("role")
    rows = size // groups
    assert blocks == 4 and sigma_in.shape[1] == 1
    packed, weight = pl.pallas_call(
        functools.partial(prepare_kernel, groups, blocks - 1),
        out_shape=(
            jax.ShapeDtypeStruct((3, size, size), F32),
            jax.ShapeDtypeStruct((rows, size), F32),
        ),
        in_specs=[SM, VM, VM, VM, VM],
        out_specs=(VM, VM),
        name="prepare",
    )(pattern, sigma_in, hamiltonian, coupling, coulomb.reshape(rows, size))
    gathered = lax.all_gather(packed, "block", axis=0, tiled=False)
    green, pieces = pl.pallas_call(
        functools.partial(green_kernel, groups),
        out_shape=(
            jax.ShapeDtypeStruct((2, 1, 1, size, size), F32),
            jax.ShapeDtypeStruct((groups, 2, rows, size), F32),
        ),
        in_specs=[VM],
        out_specs=(VM, VM),
        scratch_shapes=[
            pltpu.VMEM((2, size, 2 * size), F32),
            pltpu.VMEM((2, size, 2 * size), F32),
            pltpu.VMEM((2, 2 * size, 2 * size), F32),
            pltpu.VMEM((2, 2 * size, 2 * size), BF16),
            pltpu.VMEM((2, 2 * size, 2 * size), BF16),
            pltpu.VMEM((6, size, size), F32),
        ],
        name="green",
    )(gathered)
    spread = lax.all_to_all(pieces, ("energy", "role"), split_axis=0, concat_axis=0, tiled=True)
    screened = pl.pallas_call(
        screen_kernel,
        out_shape=jax.ShapeDtypeStruct(spread.shape, F32),
        in_specs=[SM, VM, VM],
        out_specs=VM,
        name="screen",
    )(offsets, weight, spread)
    returned = lax.all_to_all(screened, ("energy", "role"), split_axis=0, concat_axis=0, tiled=True)
    sigma_out = returned.transpose(1, 0, 2, 3).reshape(2, 1, 1, size, size)
    return green, sigma_out


def solution(mesh):
    in_specs = (
        P(None, ("energy", "role"), "block", None, None),
        P("block", None, None),
        P("block", None, None),
        P("block", ("energy", "role")),
        P(None, "block", None, None),
        P(),
    )
    out_specs = (
        P(None, ("energy", "role"), "block", None, None),
        P(None, ("energy", "role"), "block", None, None),
    )
    return jax.shard_map(body, mesh=mesh, in_specs=in_specs, out_specs=out_specs, check_vma=False)
```

```python
import functools

import jax
import jax.numpy as jnp
from jax import lax
from jax.experimental import pallas as pl
from jax.experimental.pallas import tpu as pltpu
from jax.sharding import PartitionSpec as P

ETA = 0.1
CONTACT = 0.5
HIGH = lax.Precision.HIGHEST
F32 = jnp.float32
BF16 = jnp.bfloat16

LOW = 4e-4
STEPS = 7
TRUST = 2e-5
TOL = 1e-6
MAX_SAFE = 300


def step_table(low, steps):
    rows = []
    for _ in range(steps):
        scale = 4.0 / (1.0 + low) ** 2
        rows.append((scale * (1.0 + low), scale))
        low = scale * low
    return rows, 2.0 / (1.0 + low)


def split(value):
    high = value.astype(BF16)
    return high, (value - high.astype(F32)).astype(BF16)


def dot(left, right):
    return jnp.dot(left, right, preferred_element_type=F32)


def dot3(left, right):
    return dot(left[0], right[0]) + (dot(left[0], right[1]) + dot(left[1], right[0]))


def embed(wide):
    half = wide.shape[1] // 2
    return jnp.concatenate(
        [wide, jnp.concatenate([-wide[:, half:], wide[:, :half]], axis=1)], axis=0
    )


def embed_both(parts):
    return embed(parts[0]), embed(parts[1])


def wide_eye(size):
    row = lax.broadcasted_iota(jnp.int32, (size, 2 * size), 0)
    col = lax.broadcasted_iota(jnp.int32, (size, 2 * size), 1)
    return jnp.where(row == col, 1.0, 0.0).astype(F32)


def adjoint(wide):
    half = wide.shape[1] // 2
    return jnp.concatenate([wide[:, :half].T, -wide[:, half:].T], axis=1)


def invert_many(slots, s_ref, x_ref, t_ref, e_ref, alpha_ref):
    size = s_ref.shape[1]
    table, last = step_table(LOW, STEPS)
    for slot in slots:
        value = s_ref[slot]
        parts = split(value)
        e_ref[slot, 0], e_ref[slot, 1] = embed_both(parts)
        turned = adjoint(value)
        x_ref[slot] = turned
        t_ref[slot] = dot3(parts, embed_both(split(turned)))
    for index in range(STEPS):
        lift, scale = table[index]
        for slot in slots:
            power = t_ref[slot]
            approx = x_ref[slot]
            parts = split(power)
            weights = embed_both(parts)
            if index == 0:
                size_of = jnp.abs(power[:, :size]) + jnp.abs(power[:, size:])
                bound = jnp.max(jnp.sum(size_of, axis=0, keepdims=True), axis=1, keepdims=True)
                alpha = jnp.broadcast_to(1.0 / bound, (1, 2 * size))
                alpha_ref[slot] = alpha
                t_ref[slot] = (lift * alpha) * power - (scale * alpha * alpha) * dot3(parts, weights)
                x_ref[slot] = (lift * alpha) * approx - (scale * alpha * alpha) * dot3(
                    split(approx), weights
                )
            elif index < STEPS - 1:
                t_ref[slot] = lift * power - scale * dot3(parts, weights)
                x_ref[slot] = lift * approx - scale * dot3(split(approx), weights)
            else:
                x_ref[slot] = (last * lift) * approx - (last * scale) * dot(
                    approx.astype(BF16), weights[0]
                )
    trusted = None
    contracting = None
    for slot in slots:
        approx = x_ref[slot]
        parts = split(approx)
        rest = wide_eye(size) - dot3(parts, (e_ref[slot, 0], e_ref[slot, 1]))
        rest_parts = split(rest)
        square = dot(rest_parts[0], embed(rest_parts[0]))
        better = approx + dot3(rest_parts, embed_both(parts))
        x_ref[slot] = better + dot(square.astype(BF16), embed(better.astype(BF16)))
        good = jnp.sum(square * square) < TRUST
        near = jnp.sum(rest * rest) < 0.5
        trusted = good if trusted is None else jnp.logical_and(trusted, good)
        contracting = near if contracting is None else jnp.logical_and(contracting, near)

    @pl.when(jnp.logical_not(trusted))
    def _():
        @pl.when(jnp.logical_not(contracting))
        def _():
            for slot in slots:
                x_ref[slot] = adjoint(s_ref[slot]) * alpha_ref[slot]

        def unfinished(state):
            return jnp.logical_and(state[0] < MAX_SAFE, jnp.logical_not(state[1] < TOL))

        def refine(state):
            worst = jnp.float32(0.0)
            for slot in slots:
                approx = x_ref[slot]
                parts = split(approx)
                rest = wide_eye(size) - dot3(parts, (e_ref[slot, 0], e_ref[slot, 1]))
                x_ref[slot] = approx + dot3(split(rest), embed_both(parts))
                worst = worst + jnp.sum(rest * rest)
            return state[0] + 1, worst

        lax.while_loop(unfinished, refine, (jnp.int32(0), jnp.float32(1e30)))


def prepare_kernel(total, last_block, pattern_ref, sigma_ref, ham_ref, coupling_ref, coulomb_ref, out_ref, weight_ref):
    size = ham_ref.shape[-1]
    tiles = pattern_ref.shape[-1]
    tile = size // tiles
    block = lax.axis_index("block")
    place = lax.axis_index("energy") * lax.axis_size("role") + lax.axis_index("role")

    def mask_rows(which, row_tile):
        lane = lax.broadcasted_iota(jnp.int32, (1, size), 1) // tile
        row = jnp.zeros((1, size), F32)
        for column in range(tiles):
            row = jnp.where(lane == column, pattern_ref[which, 0, row_tile, column].astype(F32), row)
        return row

    mask = jnp.concatenate(
        [jnp.broadcast_to(mask_rows(0, row_tile), (tile, size)) for row_tile in range(tiles)], axis=0
    )
    masked = ham_ref[0] * mask
    onsite = 0.5 * (masked + masked.T)
    row = lax.broadcasted_iota(jnp.int32, (size, size), 0)
    col = lax.broadcasted_iota(jnp.int32, (size, size), 1)
    number = jnp.full((size, size), place, jnp.int32).astype(F32)
    energy = -3.0 + 6.0 * number / total
    out_ref[0] = jnp.where(row == col, energy, 0.0) - onsite - sigma_ref[0, 0, 0]
    out_ref[1] = jnp.where(row == col, ETA, 0.0) - sigma_ref[1, 0, 0]
    out_ref[2] = coupling_ref[0]

    @pl.when(block == last_block)
    def _():
        square = jnp.dot(
            coupling_ref[0].T, coupling_ref[0], precision=HIGH, preferred_element_type=F32
        )
        out_ref[1] += CONTACT * square

    rows = coulomb_ref.shape[0]
    for local_row in range(rows):
        tile_row = (place * rows + local_row) // tile
        lane = lax.broadcasted_iota(jnp.int32, (1, size), 1) // tile
        line = jnp.zeros((1, size), F32)
        for column in range(tiles):
            line = jnp.where(lane == column, pattern_ref[1, 0, tile_row, column].astype(F32), line)
        value = coulomb_ref[local_row : local_row + 1] * line
        weight_ref[local_row : local_row + 1] = value * value


def green_kernel(groups, all_ref, out_ref, pieces_ref, s_ref, x_ref, t_ref, e_ref, alpha_ref, k_ref, up_ref):
    size = all_ref.shape[-1]
    own = lax.axis_index("block")
    far = own ^ 2
    low_half = own % 2 == 0
    middle = jnp.where(low_half, 1, 2)
    other = jnp.where(low_half, 3, 0)

    def base(block):
        return jnp.concatenate([all_ref[block, 0], all_ref[block, 1]], axis=1)

    for block in range(3):
        value = all_ref[block, 2]
        k_ref[block] = value
        k_ref[3 + block] = value.T

    def link(source, target):
        return k_ref[jnp.where(target > source, source, 3 + target)]

    s_ref[0] = base(middle)
    s_ref[1] = base(other)
    invert_many((0, 1), s_ref, x_ref, t_ref, e_ref, alpha_ref)

    beside = jnp.where(low_half, 2, 1)
    to_other = link(beside, other)
    both = jnp.concatenate([link(own, middle), link(far, middle)], axis=0)
    both_t = jnp.concatenate([link(middle, own), link(middle, far)], axis=1)

    def congruence(left, value, right):
        first = dot3(split(left), split(value))
        rows = jnp.concatenate([first[:, :size], first[:, size:]], axis=0)
        result = dot3(split(rows), split(right))
        count = left.shape[0]
        return result[:count], result[count:]

    real, imag = congruence(both, x_ref[0], both_t)
    o_real, o_imag = congruence(to_other, x_ref[1], link(other, beside))
    side = jnp.concatenate([o_real, o_imag], axis=1)
    beside_far = beside == far

    def wide(rows, columns):
        return jnp.concatenate([real[rows, columns], imag[rows, columns]], axis=1)

    top, bottom = slice(0, size), slice(size, 2 * size)
    s_ref[0] = base(far) - wide(bottom, bottom) - jnp.where(beside_far, side, 0.0)
    own_part = base(own) - wide(top, top) - jnp.where(beside_far, 0.0, side)
    up_ref[0] = wide(top, bottom)
    up_ref[1] = wide(bottom, top)
    s_ref[1] = own_part
    invert_many((0,), s_ref, x_ref, t_ref, e_ref, alpha_ref)
    first = dot3(split(up_ref[0]), embed_both(split(x_ref[0])))
    s_ref[0] = s_ref[1] - dot3(split(first), embed_both(split(up_ref[1])))
    invert_many((0,), s_ref, x_ref, t_ref, e_ref, alpha_ref)
    result = x_ref[0]
    out_ref[0, 0, 0] = result[:, :size]
    out_ref[1, 0, 0] = result[:, size:]
    rows = size // groups
    for group in range(groups):
        part = slice(group * rows, (group + 1) * rows)
        pieces_ref[group, 0] = result[part, :size]
        pieces_ref[group, 1] = result[part, size:]


def screen_kernel(offsets_ref, weight_ref, g_ref, out_ref):
    energies = g_ref.shape[0]
    count = offsets_ref.shape[0]
    factor = 6.0 / energies / (2.0 * 3.141592653589793) / count
    weight = weight_ref[...]

    def uses(offset):
        return lax.fori_loop(
            0, count, lambda i, total: total + jnp.where(offsets_ref[i] == offset, 1, 0), jnp.int32(0)
        )

    if energies <= 16:
        real = [g_ref[n, 0] for n in range(energies)]
        imag = [g_ref[n, 1] for n in range(energies)]
        out_real = [jnp.zeros_like(weight) for _ in range(energies)]
        out_imag = [jnp.zeros_like(weight) for _ in range(energies)]
        hits = [jnp.int32(0) for _ in range(energies)]
        for index in range(count):
            offset = offsets_ref[index]
            for d in range(energies):
                hits[d] = hits[d] + jnp.where(offset == d, 1, 0)
        for d in range(energies):
            scale = weight * (factor * hits[d].astype(F32))
            p_real = jnp.zeros_like(weight)
            p_imag = jnp.zeros_like(weight)
            for n in range(d, energies):
                p_real += real[n] * real[n - d] - imag[n] * imag[n - d]
                p_imag += real[n] * imag[n - d] + imag[n] * real[n - d]
            p_real *= scale
            p_imag *= scale
            for n in range(d, energies):
                out_real[n] += real[n - d] * p_real - imag[n - d] * p_imag
                out_imag[n] += real[n - d] * p_imag + imag[n - d] * p_real
        for n in range(energies):
            out_ref[n, 0] = out_real[n]
            out_ref[n, 1] = out_imag[n]
    else:
        out_ref[...] = jnp.zeros_like(out_ref)

        @pl.loop(0, energies)
        def _(d):
            hits = uses(d)

            @pl.when(hits > 0)
            def _():
                scale = weight * (factor * hits.astype(F32))

                def gather(n, total):
                    a, b, c, e = g_ref[n, 0], g_ref[n, 1], g_ref[n - d, 0], g_ref[n - d, 1]
                    return total[0] + a * c - b * e, total[1] + a * e + b * c

                zero = jnp.zeros_like(weight)
                p_real, p_imag = lax.fori_loop(d, energies, gather, (zero, zero))
                p_real, p_imag = p_real * scale, p_imag * scale

                @pl.loop(d, energies)
                def _(n):
                    a, b = g_ref[n - d, 0], g_ref[n - d, 1]
                    out_ref[n, 0] += a * p_real - b * p_imag
                    out_ref[n, 1] += a * p_imag + b * p_real


VM = pl.BlockSpec(memory_space=pltpu.VMEM)
SM = pl.BlockSpec(memory_space=pltpu.SMEM)


def body(sigma_in, hamiltonian, coupling, coulomb, pattern, offsets):
    size = hamiltonian.shape[-1]
    blocks = lax.axis_size("block")
    groups = lax.axis_size("energy") * lax.axis_size("role")
    rows = size // groups
    assert blocks == 4 and sigma_in.shape[1] == 1
    packed, weight = pl.pallas_call(
        functools.partial(prepare_kernel, groups, blocks - 1),
        out_shape=(
            jax.ShapeDtypeStruct((3, size, size), F32),
            jax.ShapeDtypeStruct((rows, size), F32),
        ),
        in_specs=[SM, VM, VM, VM, VM],
        out_specs=(VM, VM),
        name="prepare",
    )(pattern, sigma_in, hamiltonian, coupling, coulomb.reshape(rows, size))
    gathered = lax.all_gather(packed, "block", axis=0, tiled=False)
    green, pieces = pl.pallas_call(
        functools.partial(green_kernel, groups),
        out_shape=(
            jax.ShapeDtypeStruct((2, 1, 1, size, size), F32),
            jax.ShapeDtypeStruct((groups, 2, rows, size), F32),
        ),
        in_specs=[VM],
        out_specs=(VM, VM),
        scratch_shapes=[
            pltpu.VMEM((2, size, 2 * size), F32),
            pltpu.VMEM((2, size, 2 * size), F32),
            pltpu.VMEM((2, size, 2 * size), F32),
            pltpu.VMEM((2, 2, 2 * size, 2 * size), BF16),
            pltpu.VMEM((2, 1, 2 * size), F32),
            pltpu.VMEM((6, size, size), F32),
            pltpu.VMEM((2, size, 2 * size), F32),
        ],
        name="green",
    )(gathered)
    spread = lax.all_to_all(pieces, ("energy", "role"), split_axis=0, concat_axis=0, tiled=True)
    screened = pl.pallas_call(
        screen_kernel,
        out_shape=jax.ShapeDtypeStruct(spread.shape, F32),
        in_specs=[SM, VM, VM],
        out_specs=VM,
        name="screen",
    )(offsets, weight, spread)
    returned = lax.all_to_all(screened, ("energy", "role"), split_axis=0, concat_axis=0, tiled=True)
    sigma_out = returned.transpose(1, 0, 2, 3).reshape(2, 1, 1, size, size)
    return green, sigma_out


def solution(mesh):
    in_specs = (
        P(None, ("energy", "role"), "block", None, None),
        P("block", None, None),
        P("block", None, None),
        P("block", ("energy", "role")),
        P(None, "block", None, None),
        P(),
    )
    out_specs = (
        P(None, ("energy", "role"), "block", None, None),
        P(None, ("energy", "role"), "block", None, None),
    )
    return jax.shard_map(body, mesh=mesh, in_specs=in_specs, out_specs=out_specs, check_vma=False)
```

```python
import functools

import jax
import jax.numpy as jnp
from jax import lax
from jax.experimental import pallas as pl
from jax.experimental.pallas import tpu as pltpu
from jax.sharding import PartitionSpec as P

ETA = 0.1
CONTACT = 0.5
HIGH = lax.Precision.HIGHEST
F32 = jnp.float32
BF16 = jnp.bfloat16

LOW = 4e-4
STEPS = 7
TRUST = 2e-5
TOL = 1e-6
MAX_SAFE = 300


def step_table(low, steps):
    rows = []
    for _ in range(steps):
        scale = 4.0 / (1.0 + low) ** 2
        rows.append((scale * (1.0 + low), scale))
        low = scale * low
    return rows, 2.0 / (1.0 + low)


def split(value):
    high = value.astype(BF16)
    return high, (value - high.astype(F32)).astype(BF16)


def dot(left, right):
    return jnp.dot(left, right, preferred_element_type=F32)


def dot3(left, right):
    return dot(left[0], right[0]) + (dot(left[0], right[1]) + dot(left[1], right[0]))


def embed(wide):
    half = wide.shape[1] // 2
    return jnp.concatenate(
        [wide, jnp.concatenate([-wide[:, half:], wide[:, :half]], axis=1)], axis=0
    )


def embed_both(parts):
    return embed(parts[0]), embed(parts[1])


def wide_eye(size):
    row = lax.broadcasted_iota(jnp.int32, (size, 2 * size), 0)
    col = lax.broadcasted_iota(jnp.int32, (size, 2 * size), 1)
    return jnp.where(row == col, 1.0, 0.0).astype(F32)


def adjoint(wide):
    half = wide.shape[1] // 2
    return jnp.concatenate([wide[:, :half].T, -wide[:, half:].T], axis=1)


def invert_many(slots, s_ref, x_ref, t_ref, e_ref, alpha_ref):
    size = s_ref.shape[1]
    table, last = step_table(LOW, STEPS)
    for slot in slots:
        value = s_ref[slot]
        parts = split(value)
        e_ref[slot, 0], e_ref[slot, 1] = embed_both(parts)
        turned = adjoint(value)
        x_ref[slot] = turned
        t_ref[slot] = dot3(parts, embed_both(split(turned)))
    for index in range(STEPS):
        lift, scale = table[index]
        for slot in slots:
            power = t_ref[slot]
            approx = x_ref[slot]
            parts = split(power)
            weights = embed_both(parts)
            if index == 0:
                size_of = jnp.abs(power[:, :size]) + jnp.abs(power[:, size:])
                bound = jnp.max(jnp.sum(size_of, axis=0, keepdims=True), axis=1, keepdims=True)
                alpha = jnp.broadcast_to(1.0 / bound, (1, 2 * size))
                alpha_ref[slot] = alpha
                t_ref[slot] = (lift * alpha) * power - (scale * alpha * alpha) * dot3(parts, weights)
                x_ref[slot] = (lift * alpha) * approx - (scale * alpha * alpha) * dot3(
                    split(approx), weights
                )
            elif index < STEPS - 1:
                t_ref[slot] = lift * power - scale * dot3(parts, weights)
                x_ref[slot] = lift * approx - scale * dot3(split(approx), weights)
            else:
                x_ref[slot] = (last * lift) * approx - (last * scale) * dot(
                    approx.astype(BF16), weights[0]
                )
    trusted = None
    contracting = None
    for slot in slots:
        approx = x_ref[slot]
        parts = split(approx)
        rest = wide_eye(size) - dot3(parts, (e_ref[slot, 0], e_ref[slot, 1]))
        rest_parts = split(rest)
        square = dot(rest_parts[0], embed(rest_parts[0]))
        better = approx + dot3(rest_parts, embed_both(parts))
        x_ref[slot] = better + dot(square.astype(BF16), embed(better.astype(BF16)))
        good = jnp.sum(square * square) < TRUST
        near = jnp.sum(rest * rest) < 0.5
        trusted = good if trusted is None else jnp.logical_and(trusted, good)
        contracting = near if contracting is None else jnp.logical_and(contracting, near)

    @pl.when(jnp.logical_not(trusted))
    def _():
        @pl.when(jnp.logical_not(contracting))
        def _():
            for slot in slots:
                x_ref[slot] = adjoint(s_ref[slot]) * alpha_ref[slot]

        def unfinished(state):
            return jnp.logical_and(state[0] < MAX_SAFE, jnp.logical_not(state[1] < TOL))

        def refine(state):
            worst = jnp.float32(0.0)
            for slot in slots:
                approx = x_ref[slot]
                parts = split(approx)
                rest = wide_eye(size) - dot3(parts, (e_ref[slot, 0], e_ref[slot, 1]))
                x_ref[slot] = approx + dot3(split(rest), embed_both(parts))
                worst = worst + jnp.sum(rest * rest)
            return state[0] + 1, worst

        lax.while_loop(unfinished, refine, (jnp.int32(0), jnp.float32(1e30)))


def fetch(pairs, sems):
    copies = [pltpu.make_async_copy(source, target, sems.at[i]) for i, (source, target) in enumerate(pairs)]
    for copy in copies:
        copy.start()
    return copies


def tile_lines(pattern_ref, which, tile_row, size):
    tiles = pattern_ref.shape[-1]
    lane = lax.broadcasted_iota(jnp.int32, (1, size), 1) // (size // tiles)
    line = jnp.zeros((1, size), F32)
    for column in range(tiles):
        line = jnp.where(lane == column, pattern_ref[which, 0, tile_row, column].astype(F32), line)
    return line


def prepare_kernel(
    total, last_block, pattern_hbm, sigma_hbm, ham_hbm, coupling_hbm, coulomb_hbm,
    out_ref, weight_ref, pattern_ref, sigma_ref, ham_ref, coulomb_ref, sems,
):
    size = ham_ref.shape[-1]
    tiles = pattern_ref.shape[-1]
    tile = size // tiles
    coupling_ref = out_ref.at[2]
    copies = fetch(
        (
            (pattern_hbm, pattern_ref),
            (ham_hbm.at[0], ham_ref),
            (coupling_hbm.at[0], coupling_ref),
            (sigma_hbm.at[:, 0, 0], sigma_ref),
            (coulomb_hbm, coulomb_ref),
        ),
        sems,
    )
    block = lax.axis_index("block")
    place = lax.axis_index("energy") * lax.axis_size("role") + lax.axis_index("role")
    row = lax.broadcasted_iota(jnp.int32, (size, size), 0)
    col = lax.broadcasted_iota(jnp.int32, (size, size), 1)
    number = jnp.full((size, size), place, jnp.int32).astype(F32)
    energy = jnp.where(row == col, -3.0 + 6.0 * number / total, 0.0)
    for copy in copies:
        copy.wait()
    mask = jnp.concatenate(
        [jnp.broadcast_to(tile_lines(pattern_ref, 0, t, size), (tile, size)) for t in range(tiles)],
        axis=0,
    )
    masked = ham_ref[...] * mask
    onsite = 0.5 * (masked + masked.T)
    out_ref[0] = energy - onsite - sigma_ref[0]
    out_ref[1] = jnp.where(row == col, ETA, 0.0) - sigma_ref[1]

    @pl.when(block == last_block)
    def _():
        square = dot3(split(coupling_ref[...].T), split(coupling_ref[...]))
        out_ref[1] += CONTACT * square

    rows = coulomb_ref.shape[0]
    for local_row in range(rows):
        line = tile_lines(pattern_ref, 1, (place * rows + local_row) // tile, size)
        value = coulomb_ref[local_row : local_row + 1] * line
        weight_ref[local_row : local_row + 1] = value * value


def green_kernel(pieces, all_ref, *refs):
    out_refs, (s_ref, x_ref, t_ref, e_ref, alpha_ref, k_ref, up_ref) = refs[:-7], refs[-7:]
    size = all_ref.shape[-1]
    own = lax.axis_index("block")
    far = own ^ 2
    low_half = own % 2 == 0
    middle = jnp.where(low_half, 1, 2)
    other = jnp.where(low_half, 3, 0)

    def base(block):
        return jnp.concatenate([all_ref[block, 0], all_ref[block, 1]], axis=1)

    for block in range(3):
        value = all_ref[block, 2]
        k_ref[block] = value
        k_ref[3 + block] = value.T

    def link(source, target):
        return k_ref[jnp.where(target > source, source, 3 + target)]

    s_ref[0] = base(middle)
    s_ref[1] = base(other)
    invert_many((0, 1), s_ref, x_ref, t_ref, e_ref, alpha_ref)

    beside = jnp.where(low_half, 2, 1)
    to_other = link(beside, other)
    both = jnp.concatenate([link(own, middle), link(far, middle)], axis=0)
    both_t = jnp.concatenate([link(middle, own), link(middle, far)], axis=1)

    def congruence(left, value, right):
        first = dot3(split(left), split(value))
        rows = jnp.concatenate([first[:, :size], first[:, size:]], axis=0)
        result = dot3(split(rows), split(right))
        count = left.shape[0]
        return result[:count], result[count:]

    real, imag = congruence(both, x_ref[0], both_t)
    o_real, o_imag = congruence(to_other, x_ref[1], link(other, beside))
    side = jnp.concatenate([o_real, o_imag], axis=1)
    beside_far = beside == far

    def wide(rows, columns):
        return jnp.concatenate([real[rows, columns], imag[rows, columns]], axis=1)

    top, bottom = slice(0, size), slice(size, 2 * size)
    s_ref[0] = base(far) - wide(bottom, bottom) - jnp.where(beside_far, side, 0.0)
    own_part = base(own) - wide(top, top) - jnp.where(beside_far, 0.0, side)
    up_ref[0] = wide(top, bottom)
    up_ref[1] = wide(bottom, top)
    s_ref[1] = own_part
    invert_many((0,), s_ref, x_ref, t_ref, e_ref, alpha_ref)
    first = dot3(split(up_ref[0]), embed_both(split(x_ref[0])))
    s_ref[0] = s_ref[1] - dot3(split(first), embed_both(split(up_ref[1])))
    invert_many((0,), s_ref, x_ref, t_ref, e_ref, alpha_ref)
    if pieces == 1:
        out_refs[0][0] = x_ref[0, :, :size]
        out_refs[0][1] = x_ref[0, :, size:]
        return
    rows = size // pieces
    here = lax.axis_index("energy")
    for step in range(pieces):
        part = pl.ds(pl.multiple_of((here ^ step) * rows, rows), rows)
        out_refs[step][0] = x_ref[0, part, :size]
        out_refs[step][1] = x_ref[0, part, size:]


def join_kernel(*refs):
    out_hbm, sems = refs[-2:]
    pieces = len(refs) - 2
    rows = refs[0].shape[1]
    here = lax.axis_index("energy")
    copies = fetch(
        [
            (refs[step], out_hbm.at[:, 0, 0, pl.ds(pl.multiple_of((here ^ step) * rows, rows), rows)])
            for step in range(pieces)
        ],
        sems,
    )
    for copy in copies:
        copy.wait()


def merge_kernel(weight_ref, *refs):
    out_ref = refs[-1]
    rows = refs[0].shape[1]
    for step, ref in enumerate(refs[:-1]):
        for part in range(2):
            start = (2 * step + part) * rows
            out_ref[start : start + rows] = ref[part]
    start = 2 * rows * (len(refs) - 1)
    out_ref[start : start + weight_ref.shape[0]] = weight_ref[...]


def pair_screen_kernel(offsets_ref, own_ref, other_ref, *refs):
    out_refs, (g_ref, w_ref) = refs[:-2], refs[-2:]
    pieces = len(out_refs)
    energies = g_ref.shape[0] // 2
    rows = g_ref.shape[2]
    ways = energies // pieces
    count = offsets_ref.shape[0]
    factor = 6.0 / energies / (2.0 * 3.141592653589793) / count
    here = lax.axis_index("energy")
    role = lax.axis_index("role")
    g_ref[:energies] = jnp.zeros((energies, 2) + g_ref.shape[2:], F32)
    half = w_ref.shape[0] // ways
    start = 2 * rows * pieces
    for index, ref in ((role, own_ref), (1 - role, other_ref)):
        for step in range(pieces):
            n = energies + ways * (here ^ step) + index
            for part in range(2):
                first = (2 * step + part) * rows
                g_ref[n, part] = ref[first : first + rows]
        w_ref[pl.ds(pl.multiple_of(index * half, half), half)] = ref[start : start + half]
    hits = [jnp.int32(0) for _ in range(energies)]
    for index in range(count):
        offset = offsets_ref[index]
        for d in range(energies):
            hits[d] = hits[d] + jnp.where(offset == d, 1, 0)
    totals = [[jnp.zeros(g_ref.shape[2:], F32) for _ in range(2)] for _ in range(pieces)]
    for d in range(energies):
        p_real = jnp.zeros(g_ref.shape[2:], F32)
        p_imag = jnp.zeros(g_ref.shape[2:], F32)
        for n in range(d, energies):
            a, b = g_ref[energies + n, 0], g_ref[energies + n, 1]
            c, e = g_ref[energies + n - d, 0], g_ref[energies + n - d, 1]
            p_real += a * c - b * e
            p_imag += a * e + b * c
        scale = factor * hits[d].astype(F32)
        p_real *= scale
        p_imag *= scale
        for step in range(pieces):
            n = energies + ways * (here ^ step) + role - d
            a, b = g_ref[n, 0], g_ref[n, 1]
            totals[step][0] += a * p_real - b * p_imag
            totals[step][1] += a * p_imag + b * p_real
    weight = w_ref[...]
    for step in range(pieces):
        out_refs[step][0] = totals[step][0] * weight
        out_refs[step][1] = totals[step][1] * weight


def screen_kernel(offsets_ref, weight_ref, g_ref, out_ref):
    energies = g_ref.shape[0]
    count = offsets_ref.shape[0]
    factor = 6.0 / energies / (2.0 * 3.141592653589793) / count
    weight = weight_ref[...]

    def uses(offset):
        return lax.fori_loop(
            0, count, lambda i, total: total + jnp.where(offsets_ref[i] == offset, 1, 0), jnp.int32(0)
        )

    out_ref[...] = jnp.zeros_like(out_ref)

    @pl.loop(0, energies)
    def _(d):
        hits = uses(d)

        @pl.when(hits > 0)
        def _():
            scale = weight * (factor * hits.astype(F32))

            def gather(n, total):
                a, b, c, e = g_ref[n, 0], g_ref[n, 1], g_ref[n - d, 0], g_ref[n - d, 1]
                return total[0] + a * c - b * e, total[1] + a * e + b * c

            zero = jnp.zeros_like(weight)
            p_real, p_imag = lax.fori_loop(d, energies, gather, (zero, zero))
            p_real, p_imag = p_real * scale, p_imag * scale

            @pl.loop(d, energies)
            def _(n):
                a, b = g_ref[n - d, 0], g_ref[n - d, 1]
                out_ref[n, 0] += a * p_real - b * p_imag
                out_ref[n, 1] += a * p_imag + b * p_real


VM = pl.BlockSpec(memory_space=pltpu.VMEM)
SM = pl.BlockSpec(memory_space=pltpu.SMEM)
HB = pl.BlockSpec(memory_space=pltpu.HBM)
LIMIT = 8 * 2**20
PARAMS = pltpu.CompilerParams(vmem_limit_bytes=LIMIT)
MOST_STEPS = 8


def array(*shape):
    return jax.ShapeDtypeStruct(shape, F32)


def swap(value, axis, step):
    ways = lax.axis_size(axis)
    return lax.ppermute(value, axis, [(i, i ^ step) for i in range(ways)])


def body(sigma_in, hamiltonian, coupling, coulomb, pattern, offsets):
    size = hamiltonian.shape[-1]
    blocks = lax.axis_size("block")
    ways_energy = lax.axis_size("energy")
    ways_role = lax.axis_size("role")
    groups = ways_energy * ways_role
    rows = size // groups
    assert blocks == 4 and sigma_in.shape[1] == 1 and ways_role == 2
    packed, weight = pl.pallas_call(
        functools.partial(prepare_kernel, groups, blocks - 1),
        out_shape=(array(3, size, size), array(rows, size)),
        in_specs=[HB] * 5,
        out_specs=(VM, VM),
        scratch_shapes=[
            pltpu.SMEM(pattern.shape, jnp.int32),
            pltpu.VMEM((2, size, size), F32),
            pltpu.VMEM((size, size), F32),
            pltpu.VMEM((rows, size), F32),
            pltpu.SemaphoreType.DMA((5,)),
        ],
        name="prepare",
        compiler_params=PARAMS,
    )(*(pltpu.with_memory_space_constraint(v, pltpu.HBM) for v in (pattern, sigma_in, hamiltonian, coupling, coulomb.reshape(rows, size))))
    gathered = lax.all_gather(packed, "block", axis=0, tiled=False)
    direct = ways_energy <= MOST_STEPS
    pieces = ways_energy if direct else 1
    chunk = size // pieces
    parts = pl.pallas_call(
        functools.partial(green_kernel, pieces),
        out_shape=(array(2, chunk, size),) * pieces,
        in_specs=[VM],
        out_specs=(VM,) * pieces,
        scratch_shapes=[
            pltpu.VMEM((2, size, 2 * size), F32),
            pltpu.VMEM((2, size, 2 * size), F32),
            pltpu.VMEM((2, size, 2 * size), F32),
            pltpu.VMEM((2, 2, 2 * size, 2 * size), BF16),
            pltpu.VMEM((2, 1, 2 * size), F32),
            pltpu.VMEM((6, size, size), F32),
            pltpu.VMEM((2, size, 2 * size), F32),
        ],
        name="green",
        compiler_params=PARAMS,
    )(gathered)
    if not direct:
        green = parts[0].reshape(2, 1, 1, size, size)
        spread = lax.all_to_all(
            parts[0].reshape(2, groups, rows, size).transpose(1, 0, 2, 3),
            ("energy", "role"), split_axis=0, concat_axis=0, tiled=True,
        )
        screened = pl.pallas_call(
            screen_kernel,
            out_shape=array(*spread.shape),
            in_specs=[SM, VM, VM],
            out_specs=VM,
            name="screen",
        )(offsets, weight, spread)
        returned = lax.all_to_all(
            screened, ("energy", "role"), split_axis=0, concat_axis=0, tiled=True
        )
        return green, returned.transpose(1, 0, 2, 3).reshape(2, 1, 1, size, size)

    def join(name, values):
        return pl.pallas_call(
            join_kernel,
            out_shape=array(2, 1, 1, size, size),
            in_specs=[VM] * pieces,
            out_specs=HB,
            scratch_shapes=[pltpu.SemaphoreType.DMA((pieces,))],
            name=name,
            compiler_params=PARAMS,
        )(*values)

    arrived = [parts[0]] + [swap(parts[step], "energy", step) for step in range(1, pieces)]
    green = join("green_out", parts)
    own = pl.pallas_call(
        merge_kernel,
        out_shape=array(2 * chunk * pieces + rows, size),
        in_specs=[VM] * (pieces + 1),
        out_specs=VM,
        name="merge",
        compiler_params=PARAMS,
    )(weight, *arrived)
    other = swap(own, "role", 1)
    screened = pl.pallas_call(
        pair_screen_kernel,
        out_shape=(array(2, chunk, size),) * pieces,
        in_specs=[SM, VM, VM],
        out_specs=(VM,) * pieces,
        scratch_shapes=[
            pltpu.VMEM((2 * groups, 2, chunk, size), F32),
            pltpu.VMEM((chunk, size), F32),
        ],
        name="screen",
        compiler_params=PARAMS,
    )(offsets, own, other)
    returned = [screened[0]] + [swap(screened[step], "energy", step) for step in range(1, pieces)]
    return green, join("sigma_out", returned)


def solution(mesh):
    in_specs = (
        P(None, ("energy", "role"), "block", None, None),
        P("block", None, None),
        P("block", None, None),
        P("block", ("energy", "role")),
        P(None, "block", None, None),
        P(),
    )
    out_specs = (
        P(None, ("energy", "role"), "block", None, None),
        P(None, ("energy", "role"), "block", None, None),
    )
    return jax.shard_map(body, mesh=mesh, in_specs=in_specs, out_specs=out_specs, check_vma=False)
```

```python
import functools

import jax
import jax.numpy as jnp
from jax import lax
from jax.experimental import pallas as pl
from jax.experimental.pallas import tpu as pltpu
from jax.sharding import PartitionSpec as P

ETA = 0.1
CONTACT = 0.5
HIGH = lax.Precision.HIGHEST
F32 = jnp.float32
BF16 = jnp.bfloat16

LOW = 2.5e-4
STEPS = 7
TRUST = 2e-4
TOL = 1e-6
MAX_SAFE = 300


def step_table(low, steps):
    rows = []
    for _ in range(steps):
        scale = 4.0 / (1.0 + low) ** 2
        rows.append((scale * (1.0 + low), scale))
        low = scale * low
    return rows, 2.0 / (1.0 + low)


def split(value):
    high = value.astype(BF16)
    return high, (value - high.astype(F32)).astype(BF16)


def dot(left, right):
    return jnp.dot(left, right, preferred_element_type=F32)


def dot3(left, right):
    return dot(left[0], right[0]) + (dot(left[0], right[1]) + dot(left[1], right[0]))


def embed(wide):
    half = wide.shape[1] // 2
    return jnp.concatenate(
        [wide, jnp.concatenate([-wide[:, half:], wide[:, :half]], axis=1)], axis=0
    )


def embed_both(parts):
    return embed(parts[0]), embed(parts[1])


def wide_eye(size):
    row = lax.broadcasted_iota(jnp.int32, (size, 2 * size), 0)
    col = lax.broadcasted_iota(jnp.int32, (size, 2 * size), 1)
    return jnp.where(row == col, 1.0, 0.0).astype(F32)


def adjoint(wide):
    half = wide.shape[1] // 2
    return jnp.concatenate([wide[:, :half].T, -wide[:, half:].T], axis=1)


def rough_inverse(slots, s_ref, x_ref, t_ref, e_ref):
    size = s_ref.shape[1]
    table, last = step_table(LOW, STEPS)
    for slot in slots:
        value = s_ref[slot]
        parts = split(value)
        e_ref[slot, 0], e_ref[slot, 1] = embed_both(parts)
        turned = adjoint(value)
        x_ref[slot] = turned
        t_ref[slot] = dot3(parts, embed_both(split(turned)))
    for index in range(STEPS):
        lift, scale = table[index]
        for slot in slots:
            power = t_ref[slot]
            approx = x_ref[slot]
            parts = split(power)
            weights = embed_both(parts)
            if index == 0:
                alpha = inverse_bound(power)
                t_ref[slot] = (lift * alpha) * power - (scale * alpha * alpha) * dot3(parts, weights)
                x_ref[slot] = (lift * alpha) * approx - (scale * alpha * alpha) * dot3(
                    split(approx), weights
                )
            elif index < STEPS - 1:
                t_ref[slot] = lift * power - scale * dot3(parts, weights)
                x_ref[slot] = lift * approx - scale * dot3(split(approx), weights)
            else:
                x_ref[slot] = (last * lift) * approx - (last * scale) * dot(
                    approx.astype(BF16), weights[0]
                )


def inverse_bound(normal):
    size = normal.shape[0]
    sizes = jnp.sqrt(normal[:, :size] ** 2 + normal[:, size:] ** 2)
    bound = jnp.max(jnp.sum(sizes, axis=0, keepdims=True), axis=1, keepdims=True)
    return jnp.broadcast_to(1.0 / bound, (1, 2 * size))


def correction(slot, x_ref, e_ref):
    approx = x_ref[slot]
    parts = split(approx)
    rest = wide_eye(approx.shape[0]) - dot3(parts, (e_ref[slot, 0], e_ref[slot, 1]))
    rest_parts = split(rest)
    square = dot(rest_parts[0], embed(rest_parts[0]))
    better = approx + dot3(rest_parts, embed_both(parts))
    return better, square, jnp.sum(square * square) < TRUST


def safe_inverse(slot, s_ref, x_ref, e_ref):
    value = s_ref[slot]
    parts = split(value)
    e_ref[slot, 0], e_ref[slot, 1] = embed_both(parts)
    turned = adjoint(value)
    x_ref[slot] = turned * inverse_bound(dot3(parts, embed_both(split(turned))))

    def unfinished(state):
        return jnp.logical_and(state[0] < MAX_SAFE, jnp.logical_not(state[1] < TOL))

    def refine(state):
        approx = x_ref[slot]
        parts = split(approx)
        rest = wide_eye(approx.shape[0]) - dot3(parts, (e_ref[slot, 0], e_ref[slot, 1]))
        x_ref[slot] = approx + dot3(split(rest), embed_both(parts))
        return state[0] + 1, jnp.sum(rest * rest)

    lax.while_loop(unfinished, refine, (jnp.int32(0), jnp.float32(1e30)))


def stack_parts(wide):
    half = wide.shape[1] // 2
    return jnp.concatenate([wide[:, :half], wide[:, half:]], axis=0)


def right_real(wide, matrix):
    rows = wide.shape[0]
    result = dot3(split(stack_parts(wide)), split(matrix))
    return jnp.concatenate([result[:rows], result[rows:]], axis=1)


def congruence(left, better, square, right):
    first = dot(left.astype(BF16), square.astype(BF16))
    size = left.shape[1]
    first = jnp.concatenate([left + first[:, :size], first[:, size:]], axis=1)
    return dot3(split(first), embed_both(split(right_real(better, right))))


def fetch(pairs, sems):
    copies = [pltpu.make_async_copy(source, target, sems.at[i]) for i, (source, target) in enumerate(pairs)]
    for copy in copies:
        copy.start()
    return copies


def tile_lines(pattern_ref, which, tile_row, size):
    tiles = pattern_ref.shape[-1]
    lane = lax.broadcasted_iota(jnp.int32, (1, size), 1) // (size // tiles)
    line = jnp.zeros((1, size), F32)
    for column in range(tiles):
        line = jnp.where(lane == column, pattern_ref[which, 0, tile_row, column].astype(F32), line)
    return line


def prepare_kernel(
    total, last_block, pattern_hbm, sigma_hbm, ham_hbm, coupling_hbm, coulomb_hbm,
    out_ref, weight_ref, pattern_ref, sigma_ref, ham_ref, coulomb_ref, sems,
):
    size = ham_ref.shape[-1]
    tiles = pattern_ref.shape[-1]
    tile = size // tiles
    coupling_ref = out_ref.at[2]
    copies = fetch(
        (
            (pattern_hbm, pattern_ref),
            (ham_hbm.at[0], ham_ref),
            (coupling_hbm.at[0], coupling_ref),
            (sigma_hbm.at[:, 0, 0], sigma_ref),
            (coulomb_hbm, coulomb_ref),
        ),
        sems,
    )
    block = lax.axis_index("block")
    place = lax.axis_index("energy") * lax.axis_size("role") + lax.axis_index("role")
    row = lax.broadcasted_iota(jnp.int32, (size, size), 0)
    col = lax.broadcasted_iota(jnp.int32, (size, size), 1)
    number = jnp.full((size, size), place, jnp.int32).astype(F32)
    energy = jnp.where(row == col, -3.0 + 6.0 * number / total, 0.0)
    for copy in copies:
        copy.wait()
    mask = jnp.concatenate(
        [jnp.broadcast_to(tile_lines(pattern_ref, 0, t, size), (tile, size)) for t in range(tiles)],
        axis=0,
    )
    masked = ham_ref[...] * mask
    onsite = 0.5 * (masked + masked.T)
    out_ref[0] = energy - onsite - sigma_ref[0]
    out_ref[1] = jnp.where(row == col, ETA, 0.0) - sigma_ref[1]

    @pl.when(block == last_block)
    def _():
        square = dot3(split(coupling_ref[...].T), split(coupling_ref[...]))
        out_ref[1] += CONTACT * square

    rows = coulomb_ref.shape[0]
    for local_row in range(rows):
        line = tile_lines(pattern_ref, 1, (place * rows + local_row) // tile, size)
        value = coulomb_ref[local_row : local_row + 1] * line
        weight_ref[local_row : local_row + 1] = value * value


def green_kernel(pieces, all_ref, *refs):
    out_refs, (s_ref, x_ref, t_ref, e_ref, k_ref, up_ref) = refs[:-6], refs[-6:]
    size = all_ref.shape[-1]
    own = lax.axis_index("block")
    far = own ^ 2
    low_half = own % 2 == 0
    middle = jnp.where(low_half, 1, 2)
    other = jnp.where(low_half, 3, 0)

    def base(block):
        return jnp.concatenate([all_ref[block, 0], all_ref[block, 1]], axis=1)

    for block in range(3):
        value = all_ref[block, 2]
        k_ref[block] = value
        k_ref[3 + block] = value.T

    def link(source, target):
        return k_ref[jnp.where(target > source, source, 3 + target)]

    beside = jnp.where(low_half, 2, 1)
    beside_far = beside == far
    top, bottom = slice(0, size), slice(size, 2 * size)

    def reduce(corner, side):
        def wide(rows, columns):
            return jnp.concatenate([corner[rows, columns], corner[rows, 2 * size :][:, columns]], axis=1)

        s_ref[0] = base(far) - wide(bottom, bottom) - jnp.where(beside_far, side, 0.0)
        s_ref[1] = base(own) - wide(top, top) - jnp.where(beside_far, 0.0, side)
        up_ref[0] = wide(top, bottom)
        up_ref[1] = wide(bottom, top)

    def links():
        both = jnp.concatenate([link(own, middle), link(far, middle)], axis=0)
        both_t = jnp.concatenate([link(middle, own), link(middle, far)], axis=1)
        return both, both_t, link(beside, other), link(other, beside)

    s_ref[0] = base(middle)
    s_ref[1] = base(other)
    rough_inverse((0, 1), s_ref, x_ref, t_ref, e_ref)
    both, both_t, out_link, in_link = links()
    better, square, good_middle = correction(0, x_ref, e_ref)
    corner = congruence(both, better, square, both_t)
    better, square, good_other = correction(1, x_ref, e_ref)
    reduce(corner, congruence(out_link, better, square, in_link))

    rough_inverse((0,), s_ref, x_ref, t_ref, e_ref)
    better, square, good_far = correction(0, x_ref, e_ref)
    up = up_ref[0]
    left = up + dot(up.astype(BF16), embed(square.astype(BF16)))
    right = dot3(split(better), embed_both(split(up_ref[1])))
    s_ref[0] = s_ref[1] - dot3(split(left), embed_both(split(right)))

    rough_inverse((0,), s_ref, x_ref, t_ref, e_ref)
    better, square, good_own = correction(0, x_ref, e_ref)
    x_ref[0] = better + dot(square.astype(BF16), embed(better.astype(BF16)))
    good = jnp.logical_and(jnp.logical_and(good_middle, good_other), jnp.logical_and(good_far, good_own))

    @pl.when(jnp.logical_not(good))
    def _():
        zero = jnp.zeros((size, 2 * size), F32)
        both, both_t, out_link, in_link = links()
        s_ref[0] = base(middle)
        safe_inverse(0, s_ref, x_ref, e_ref)
        s_ref[1] = base(other)
        safe_inverse(1, s_ref, x_ref, e_ref)
        reduce(
            congruence(both, x_ref[0], zero, both_t), congruence(out_link, x_ref[1], zero, in_link)
        )
        safe_inverse(0, s_ref, x_ref, e_ref)
        first = dot3(split(up_ref[0]), embed_both(split(x_ref[0])))
        s_ref[0] = s_ref[1] - dot3(split(first), embed_both(split(up_ref[1])))
        safe_inverse(0, s_ref, x_ref, e_ref)

    if pieces == 1:
        out_refs[0][0] = x_ref[0, :, :size]
        out_refs[0][1] = x_ref[0, :, size:]
        return
    rows = size // pieces
    here = lax.axis_index("energy")
    for step in range(pieces):
        part = pl.ds(pl.multiple_of((here ^ step) * rows, rows), rows)
        out_refs[step][0] = x_ref[0, part, :size]
        out_refs[step][1] = x_ref[0, part, size:]


def join_kernel(*refs):
    out_hbm, sems = refs[-2:]
    pieces = len(refs) - 2
    rows = refs[0].shape[1]
    here = lax.axis_index("energy")
    copies = fetch(
        [
            (refs[pieces - 1 - step], out_hbm.at[:, 0, 0, pl.ds(pl.multiple_of((here ^ step) * rows, rows), rows)])
            for step in range(pieces)
        ],
        sems,
    )
    for copy in copies:
        copy.wait()


def merge_kernel(weight_ref, *refs):
    out_ref = refs[-1]
    rows = refs[0].shape[1]
    for step, ref in enumerate(refs[:-1][::-1]):
        for part in range(2):
            start = (2 * step + part) * rows
            out_ref[start : start + rows] = ref[part]
    start = 2 * rows * (len(refs) - 1)
    out_ref[start : start + weight_ref.shape[0]] = weight_ref[...]


def pair_screen_kernel(hits_ref, own_ref, other_ref, *refs):
    out_refs, (g_ref, w_ref) = refs[:-2], refs[-2:]
    pieces = len(out_refs)
    energies = g_ref.shape[0] // 2
    rows = g_ref.shape[2]
    ways = energies // pieces
    here = lax.axis_index("energy")
    role = lax.axis_index("role")
    g_ref[:energies] = jnp.zeros((energies, 2) + g_ref.shape[2:], F32)
    half = w_ref.shape[0] // ways
    start = 2 * rows * pieces
    for index, ref in ((role, own_ref), (1 - role, other_ref)):
        for step in range(pieces):
            n = energies + ways * (here ^ step) + index
            for part in range(2):
                first = (2 * step + part) * rows
                g_ref[n, part] = ref[first : first + rows]
        w_ref[pl.ds(pl.multiple_of(index * half, half), half)] = ref[start : start + half]
    totals = [[jnp.zeros(g_ref.shape[2:], F32) for _ in range(2)] for _ in range(pieces)]
    for d in range(energies):
        p_real = jnp.zeros(g_ref.shape[2:], F32)
        p_imag = jnp.zeros(g_ref.shape[2:], F32)
        for n in range(d, energies):
            a, b = g_ref[energies + n, 0], g_ref[energies + n, 1]
            c, e = g_ref[energies + n - d, 0], g_ref[energies + n - d, 1]
            p_real += a * c - b * e
            p_imag += a * e + b * c
        scale = hits_ref[d : d + 1]
        p_real *= scale
        p_imag *= scale
        for step in range(pieces):
            n = energies + ways * (here ^ step) + role - d
            a, b = g_ref[n, 0], g_ref[n, 1]
            totals[step][0] += a * p_real - b * p_imag
            totals[step][1] += a * p_imag + b * p_real
    weight = w_ref[...]
    for step in range(pieces):
        out_refs[step][0] = totals[step][0] * weight
        out_refs[step][1] = totals[step][1] * weight


def screen_kernel(offsets_ref, weight_ref, g_ref, out_ref):
    energies = g_ref.shape[0]
    count = offsets_ref.shape[0]
    factor = 6.0 / energies / (2.0 * 3.141592653589793) / count
    weight = weight_ref[...]

    def uses(offset):
        return lax.fori_loop(
            0, count, lambda i, total: total + jnp.where(offsets_ref[i] == offset, 1, 0), jnp.int32(0)
        )

    out_ref[...] = jnp.zeros_like(out_ref)

    @pl.loop(0, energies)
    def _(d):
        hits = uses(d)

        @pl.when(hits > 0)
        def _():
            scale = weight * (factor * hits.astype(F32))

            def gather(n, total):
                a, b, c, e = g_ref[n, 0], g_ref[n, 1], g_ref[n - d, 0], g_ref[n - d, 1]
                return total[0] + a * c - b * e, total[1] + a * e + b * c

            zero = jnp.zeros_like(weight)
            p_real, p_imag = lax.fori_loop(d, energies, gather, (zero, zero))
            p_real, p_imag = p_real * scale, p_imag * scale

            @pl.loop(d, energies)
            def _(n):
                a, b = g_ref[n - d, 0], g_ref[n - d, 1]
                out_ref[n, 0] += a * p_real - b * p_imag
                out_ref[n, 1] += a * p_imag + b * p_real


VM = pl.BlockSpec(memory_space=pltpu.VMEM)
SM = pl.BlockSpec(memory_space=pltpu.SMEM)
HB = pl.BlockSpec(memory_space=pltpu.HBM)
LIMIT = 8 * 2**20
PARAMS = pltpu.CompilerParams(vmem_limit_bytes=LIMIT)
MOST_STEPS = 8


def array(*shape):
    return jax.ShapeDtypeStruct(shape, F32)


def swap(value, axis, step):
    ways = lax.axis_size(axis)
    return lax.ppermute(value, axis, [(i, i ^ step) for i in range(ways)])


def exchange(values):
    result = list(values)
    for step in reversed(range(1, len(values))):
        result[step] = swap(values[step], "energy", step)
    return result


def body(sigma_in, hamiltonian, coupling, coulomb, pattern, offsets):
    size = hamiltonian.shape[-1]
    blocks = lax.axis_size("block")
    ways_energy = lax.axis_size("energy")
    ways_role = lax.axis_size("role")
    groups = ways_energy * ways_role
    rows = size // groups
    assert blocks == 4 and sigma_in.shape[1] == 1 and ways_role == 2
    packed, weight = pl.pallas_call(
        functools.partial(prepare_kernel, groups, blocks - 1),
        out_shape=(array(3, size, size), array(rows, size)),
        in_specs=[HB] * 5,
        out_specs=(VM, VM),
        scratch_shapes=[
            pltpu.SMEM(pattern.shape, jnp.int32),
            pltpu.VMEM((2, size, size), F32),
            pltpu.VMEM((size, size), F32),
            pltpu.VMEM((rows, size), F32),
            pltpu.SemaphoreType.DMA((5,)),
        ],
        name="prepare",
        compiler_params=PARAMS,
    )(*(pltpu.with_memory_space_constraint(v, pltpu.HBM) for v in (pattern, sigma_in, hamiltonian, coupling, coulomb.reshape(rows, size))))
    gathered = lax.all_gather(packed, "block", axis=0, tiled=False)
    direct = ways_energy <= MOST_STEPS
    pieces = ways_energy if direct else 1
    chunk = size // pieces
    parts = pl.pallas_call(
        functools.partial(green_kernel, pieces),
        out_shape=(array(2, chunk, size),) * pieces,
        in_specs=[VM],
        out_specs=(VM,) * pieces,
        scratch_shapes=[
            pltpu.VMEM((2, size, 2 * size), F32),
            pltpu.VMEM((2, size, 2 * size), F32),
            pltpu.VMEM((2, size, 2 * size), F32),
            pltpu.VMEM((2, 2, 2 * size, 2 * size), BF16),
            pltpu.VMEM((6, size, size), F32),
            pltpu.VMEM((2, size, 2 * size), F32),
        ],
        name="green",
        compiler_params=PARAMS,
    )(gathered)
    if not direct:
        green = parts[0].reshape(2, 1, 1, size, size)
        spread = lax.all_to_all(
            parts[0].reshape(2, groups, rows, size).transpose(1, 0, 2, 3),
            ("energy", "role"), split_axis=0, concat_axis=0, tiled=True,
        )
        screened = pl.pallas_call(
            screen_kernel,
            out_shape=array(*spread.shape),
            in_specs=[SM, VM, VM],
            out_specs=VM,
            name="screen",
        )(offsets, weight, spread)
        returned = lax.all_to_all(
            screened, ("energy", "role"), split_axis=0, concat_axis=0, tiled=True
        )
        return green, returned.transpose(1, 0, 2, 3).reshape(2, 1, 1, size, size)

    def join(name, values):
        return pl.pallas_call(
            join_kernel,
            out_shape=array(2, 1, 1, size, size),
            in_specs=[VM] * pieces,
            out_specs=HB,
            scratch_shapes=[pltpu.SemaphoreType.DMA((pieces,))],
            name=name,
            compiler_params=PARAMS,
        )(*values[::-1])

    arrived = exchange(parts)
    green = join("green_out", parts)
    own = pl.pallas_call(
        merge_kernel,
        out_shape=array(2 * chunk * pieces + rows, size),
        in_specs=[VM] * (pieces + 1),
        out_specs=VM,
        name="merge",
        compiler_params=PARAMS,
    )(weight, *arrived[::-1])
    other = swap(own, "role", 1)
    factor = 6.0 / groups / (2.0 * 3.141592653589793) / offsets.shape[0]
    hits = jnp.sum(offsets[None, :] == jnp.arange(groups)[:, None], axis=1, keepdims=True)
    hits = jnp.broadcast_to(factor * hits.astype(F32), (groups, size))
    screened = pl.pallas_call(
        pair_screen_kernel,
        out_shape=(array(2, chunk, size),) * pieces,
        in_specs=[VM, VM, VM],
        out_specs=(VM,) * pieces,
        scratch_shapes=[
            pltpu.VMEM((2 * groups, 2, chunk, size), F32),
            pltpu.VMEM((chunk, size), F32),
        ],
        name="screen",
        compiler_params=PARAMS,
    )(hits, own, other)
    return green, join("sigma_out", exchange(screened))


def solution(mesh):
    in_specs = (
        P(None, ("energy", "role"), "block", None, None),
        P("block", None, None),
        P("block", None, None),
        P("block", ("energy", "role")),
        P(None, "block", None, None),
        P(),
    )
    out_specs = (
        P(None, ("energy", "role"), "block", None, None),
        P(None, ("energy", "role"), "block", None, None),
    )
    return jax.shard_map(body, mesh=mesh, in_specs=in_specs, out_specs=out_specs, check_vma=False)
```

```python
import functools

import jax
import jax.numpy as jnp
from jax import lax
from jax.experimental import pallas as pl
from jax.experimental.pallas import tpu as pltpu
from jax.sharding import PartitionSpec as P

ETA = 0.1
CONTACT = 0.5
HIGH = lax.Precision.HIGHEST
F32 = jnp.float32
BF16 = jnp.bfloat16

LOW = 2.5e-4
STEPS = 7
TRUST = 2e-4
TOL = 1e-6
MAX_SAFE = 300


def step_table(low, steps):
    rows = []
    for _ in range(steps):
        scale = 4.0 / (1.0 + low) ** 2
        rows.append((scale * (1.0 + low), scale))
        low = scale * low
    return rows, 2.0 / (1.0 + low)


def split(value):
    high = value.astype(BF16)
    return high, (value - high.astype(F32)).astype(BF16)


def dot(left, right):
    return jnp.dot(left, right, preferred_element_type=F32)


def dot_turned(left, right):
    return lax.dot_general(left, right, (((1,), (1,)), ((), ())), preferred_element_type=F32)


def normal_matrix(parts, weights):
    return dot_turned(parts[0], weights[0]) + (
        dot_turned(parts[0], weights[1]) + dot_turned(parts[1], weights[0])
    )


def dot3(left, right):
    rows = left[0].shape[0]
    both = dot(jnp.concatenate([left[0], left[1]], axis=0), right[0])
    return (both[:rows] + both[rows:]) + dot(left[0], right[1])


def embed(wide):
    half = wide.shape[1] // 2
    return jnp.concatenate(
        [wide, jnp.concatenate([-wide[:, half:], wide[:, :half]], axis=1)], axis=0
    )


def embed_both(parts):
    return embed(parts[0]), embed(parts[1])


def wide_eye(size):
    row = lax.broadcasted_iota(jnp.int32, (size, 2 * size), 0)
    col = lax.broadcasted_iota(jnp.int32, (size, 2 * size), 1)
    return jnp.where(row == col, 1.0, 0.0).astype(F32)


def adjoint(wide):
    half = wide.shape[1] // 2
    return jnp.concatenate([wide[:, :half].T, -wide[:, half:].T], axis=1)


def rough_inverse(slots, s_ref, x_ref, t_ref, e_ref):
    size = s_ref.shape[1]
    table, last = step_table(LOW, STEPS)
    for slot in slots:
        value = s_ref[slot]
        parts = split(value)
        weights = embed_both(parts)
        e_ref[slot, 0], e_ref[slot, 1] = weights
        t_ref[slot] = normal_matrix(parts, weights)
        x_ref[slot] = adjoint(value)
    for index in range(STEPS):
        lift, scale = table[index]
        for slot in slots:
            power = t_ref[slot]
            approx = x_ref[slot]
            parts = split(power)
            weights = embed_both(parts)
            if index == 0:
                alpha = inverse_bound(power)
                t_ref[slot] = (lift * alpha) * power - (scale * alpha * alpha) * dot3(parts, weights)
                x_ref[slot] = (lift * alpha) * approx - (scale * alpha * alpha) * dot3(
                    split(approx), weights
                )
            elif index < STEPS - 1:
                t_ref[slot] = lift * power - scale * dot3(parts, weights)
                x_ref[slot] = lift * approx - scale * dot3(split(approx), weights)
            else:
                x_ref[slot] = (last * lift) * approx - (last * scale) * dot(
                    approx.astype(BF16), weights[0]
                )


def inverse_bound(normal):
    size = normal.shape[0]
    sizes = jnp.sqrt(normal[:, :size] ** 2 + normal[:, size:] ** 2)
    bound = jnp.max(jnp.sum(sizes, axis=0, keepdims=True), axis=1, keepdims=True)
    return jnp.broadcast_to(1.0 / bound, (1, 2 * size))


def correction(slot, x_ref, e_ref):
    approx = x_ref[slot]
    parts = split(approx)
    rest = wide_eye(approx.shape[0]) - dot3(parts, (e_ref[slot, 0], e_ref[slot, 1]))
    rest_parts = split(rest)
    square = dot(rest_parts[0], embed(rest_parts[0]))
    better = approx + dot3(rest_parts, embed_both(parts))
    return better, square


def small(square):
    return jnp.sum(square * square) < TRUST


def safe_inverse(slot, s_ref, x_ref, e_ref):
    value = s_ref[slot]
    parts = split(value)
    weights = embed_both(parts)
    e_ref[slot, 0], e_ref[slot, 1] = weights
    x_ref[slot] = adjoint(value) * inverse_bound(normal_matrix(parts, weights))

    def unfinished(state):
        return jnp.logical_and(state[0] < MAX_SAFE, jnp.logical_not(state[1] < TOL))

    def refine(state):
        approx = x_ref[slot]
        parts = split(approx)
        rest = wide_eye(approx.shape[0]) - dot3(parts, (e_ref[slot, 0], e_ref[slot, 1]))
        x_ref[slot] = approx + dot3(split(rest), embed_both(parts))
        return state[0] + 1, jnp.sum(rest * rest)

    lax.while_loop(unfinished, refine, (jnp.int32(0), jnp.float32(1e30)))


def stack_parts(wide):
    half = wide.shape[1] // 2
    return jnp.concatenate([wide[:, :half], wide[:, half:]], axis=0)


def right_real(wide, matrix):
    rows = wide.shape[0]
    result = dot3(split(stack_parts(wide)), split(matrix))
    return jnp.concatenate([result[:rows], result[rows:]], axis=1)


def congruence(left, better, square, right):
    first = dot(left.astype(BF16), square.astype(BF16))
    size = left.shape[1]
    first = jnp.concatenate([left + first[:, :size], first[:, size:]], axis=1)
    return dot3(split(first), embed_both(split(right_real(better, right))))


def fetch(pairs, sems):
    copies = [pltpu.make_async_copy(source, target, sems.at[i]) for i, (source, target) in enumerate(pairs)]
    for copy in copies:
        copy.start()
    return copies


def tile_lines(pattern_ref, which, tile_row, size):
    tiles = pattern_ref.shape[-1]
    lane = lax.broadcasted_iota(jnp.int32, (1, size), 1) // (size // tiles)
    line = jnp.zeros((1, size), F32)
    for column in range(tiles):
        line = jnp.where(lane == column, pattern_ref[which, 0, tile_row, column].astype(F32), line)
    return line


def prepare_kernel(
    total, last_block, pattern_hbm, sigma_hbm, ham_hbm, coupling_hbm,
    out_ref, pattern_ref, sigma_ref, ham_ref, coupling_ref, sems,
):
    size = ham_ref.shape[-1]
    tiles = pattern_ref.shape[-1]
    tile = size // tiles
    copies = fetch(
        (
            (pattern_hbm, pattern_ref),
            (ham_hbm.at[0], ham_ref),
            (coupling_hbm.at[0], coupling_ref),
            (sigma_hbm.at[:, 0, 0], sigma_ref),
        ),
        sems,
    )
    block = lax.axis_index("block")
    role = lax.axis_index("role")
    place = lax.axis_index("energy") * lax.axis_size("role") + role
    row = lax.broadcasted_iota(jnp.int32, (size, size), 0)
    col = lax.broadcasted_iota(jnp.int32, (size, size), 1)
    number = jnp.full((size, size), place, jnp.int32).astype(F32)
    energy = jnp.where(row == col, -3.0 + 6.0 * number / total, 0.0)
    for copy in copies:
        copy.wait()
    mask = jnp.concatenate(
        [jnp.broadcast_to(tile_lines(pattern_ref, 0, t, size), (tile, size)) for t in range(tiles)],
        axis=0,
    )
    masked = ham_ref[...] * mask
    onsite = 0.5 * (masked + masked.T)
    out_ref[:size] = energy - onsite - sigma_ref[0]
    out_ref[size : 2 * size] = jnp.where(row == col, ETA, 0.0) - sigma_ref[1]
    share = out_ref.shape[0] - 2 * size
    out_ref[2 * size :] = coupling_ref[pl.ds(pl.multiple_of(role * share, share), share)]

    @pl.when(block == last_block)
    def _():
        square = dot3(split(coupling_ref[...].T), split(coupling_ref[...]))
        out_ref[size : 2 * size] += CONTACT * square


def weight_kernel(pattern_ref, coulomb_ref, weight_ref):
    rows, size = coulomb_ref.shape
    tile = size // pattern_ref.shape[-1]
    place = lax.axis_index("energy") * lax.axis_size("role") + lax.axis_index("role")
    for local_row in range(rows):
        line = tile_lines(pattern_ref, 1, (place * rows + local_row) // tile, size)
        value = coulomb_ref[local_row : local_row + 1] * line
        weight_ref[local_row : local_row + 1] = value * value


def share_kernel(all_ref, out_ref):
    first = all_ref.shape[1] - out_ref.shape[1]
    for block in range(out_ref.shape[0]):
        out_ref[block] = all_ref[block, first:]


def neighbours():
    own = lax.axis_index("block")
    low_half = own % 2 == 0
    return own, own ^ 2, jnp.where(low_half, 1, 2), jnp.where(low_half, 3, 0)


def wide_base(all_ref, block):
    size = all_ref.shape[-1]
    return jnp.concatenate([all_ref[block, :size], all_ref[block, size : 2 * size]], axis=1)


def side_kernel(all_ref, better_ref, square_ref, s_ref, x_ref, t_ref, e_ref):
    _, _, middle, other = neighbours()
    s_ref[0] = wide_base(all_ref, middle)
    s_ref[1] = wide_base(all_ref, other)
    rough_inverse((0, 1), s_ref, x_ref, t_ref, e_ref)
    for slot in range(2):
        better_ref[slot], square_ref[slot] = correction(slot, x_ref, e_ref)


def green_kernel(pieces, all_ref, mine_ref, theirs_ref, better_ref, square_ref, *refs):
    out_refs, (s_ref, x_ref, t_ref, e_ref, k_ref, up_ref) = refs[:-6], refs[-6:]
    size = all_ref.shape[-1]
    own, far, middle, other = neighbours()
    role = lax.axis_index("role")

    def base(block):
        return wide_base(all_ref, block)

    share = mine_ref.shape[1]
    for block in range(3):
        for index, ref in ((role, mine_ref), (1 - role, theirs_ref)):
            k_ref[block, pl.ds(pl.multiple_of(index * share, share), share)] = ref[block]
        k_ref[3 + block] = k_ref[block].T

    def link(source, target):
        return k_ref[jnp.where(target > source, source, 3 + target)]

    beside = jnp.where(own % 2 == 0, 2, 1)
    beside_far = beside == far
    top, bottom = slice(0, size), slice(size, 2 * size)

    def reduce(corner, side):
        def wide(rows, columns):
            return jnp.concatenate([corner[rows, columns], corner[rows, 2 * size :][:, columns]], axis=1)

        s_ref[0] = base(far) - wide(bottom, bottom) - jnp.where(beside_far, side, 0.0)
        s_ref[1] = base(own) - wide(top, top) - jnp.where(beside_far, 0.0, side)
        up_ref[0] = wide(top, bottom)
        up_ref[1] = wide(bottom, top)

    def links():
        both = jnp.concatenate([link(own, middle), link(far, middle)], axis=0)
        both_t = jnp.concatenate([link(middle, own), link(middle, far)], axis=1)
        return both, both_t, link(beside, other), link(other, beside)

    both, both_t, out_link, in_link = links()
    corner = congruence(both, better_ref[0], square_ref[0], both_t)
    reduce(corner, congruence(out_link, better_ref[1], square_ref[1], in_link))
    good = jnp.logical_and(small(square_ref[0]), small(square_ref[1]))

    rough_inverse((0,), s_ref, x_ref, t_ref, e_ref)
    better, square = correction(0, x_ref, e_ref)
    good = jnp.logical_and(good, small(square))
    up = up_ref[0]
    left = up + dot(up.astype(BF16), embed(square.astype(BF16)))
    right = dot3(split(better), embed_both(split(up_ref[1])))
    s_ref[0] = s_ref[1] - dot3(split(left), embed_both(split(right)))

    rough_inverse((0,), s_ref, x_ref, t_ref, e_ref)
    better, square = correction(0, x_ref, e_ref)
    good = jnp.logical_and(good, small(square))
    x_ref[0] = better + dot(square.astype(BF16), embed(better.astype(BF16)))

    @pl.when(jnp.logical_not(good))
    def _():
        zero = jnp.zeros((size, 2 * size), F32)
        both, both_t, out_link, in_link = links()
        s_ref[0] = base(middle)
        safe_inverse(0, s_ref, x_ref, e_ref)
        s_ref[1] = base(other)
        safe_inverse(1, s_ref, x_ref, e_ref)
        reduce(
            congruence(both, x_ref[0], zero, both_t), congruence(out_link, x_ref[1], zero, in_link)
        )
        safe_inverse(0, s_ref, x_ref, e_ref)
        first = dot3(split(up_ref[0]), embed_both(split(x_ref[0])))
        s_ref[0] = s_ref[1] - dot3(split(first), embed_both(split(up_ref[1])))
        safe_inverse(0, s_ref, x_ref, e_ref)

    if pieces == 1:
        out_refs[0][0] = x_ref[0, :, :size]
        out_refs[0][1] = x_ref[0, :, size:]
        return
    rows = size // pieces
    here = lax.axis_index("energy")
    for step in range(pieces):
        part = pl.ds(pl.multiple_of((here ^ step) * rows, rows), rows)
        out_refs[step][0] = x_ref[0, part, :size]
        out_refs[step][1] = x_ref[0, part, size:]


def join_kernel(*refs):
    out_hbm, sems = refs[-2:]
    pieces = len(refs) - 2
    rows = refs[0].shape[1]
    here = lax.axis_index("energy")
    copies = fetch(
        [
            (refs[pieces - 1 - step], out_hbm.at[:, 0, 0, pl.ds(pl.multiple_of((here ^ step) * rows, rows), rows)])
            for step in range(pieces)
        ],
        sems,
    )
    for copy in copies:
        copy.wait()


def merge_kernel(weight_ref, *refs):
    out_ref = refs[-1]
    rows = refs[0].shape[1]
    for step, ref in enumerate(refs[:-1][::-1]):
        for part in range(2):
            start = (2 * step + part) * rows
            out_ref[start : start + rows] = ref[part]
    start = 2 * rows * (len(refs) - 1)
    out_ref[start : start + weight_ref.shape[0]] = weight_ref[...]


def pair_screen_kernel(hits_ref, own_ref, other_ref, *refs):
    out_refs, (g_ref, w_ref) = refs[:-2], refs[-2:]
    pieces = len(out_refs)
    energies = g_ref.shape[0] // 2
    rows = g_ref.shape[2]
    ways = energies // pieces
    here = lax.axis_index("energy")
    role = lax.axis_index("role")
    g_ref[:energies] = jnp.zeros((energies, 2) + g_ref.shape[2:], F32)
    half = w_ref.shape[0] // ways
    start = 2 * rows * pieces
    for index, ref in ((role, own_ref), (1 - role, other_ref)):
        for step in range(pieces):
            n = energies + ways * (here ^ step) + (index if step == 0 else 1 - index)
            for part in range(2):
                first = (2 * step + part) * rows
                g_ref[n, part] = ref[first : first + rows]
        w_ref[pl.ds(pl.multiple_of(index * half, half), half)] = ref[start : start + half]
    totals = [[jnp.zeros(g_ref.shape[2:], F32) for _ in range(2)] for _ in range(pieces)]
    for d in range(energies):
        p_real = jnp.zeros(g_ref.shape[2:], F32)
        p_imag = jnp.zeros(g_ref.shape[2:], F32)
        for n in range(d, energies):
            a, b = g_ref[energies + n, 0], g_ref[energies + n, 1]
            c, e = g_ref[energies + n - d, 0], g_ref[energies + n - d, 1]
            p_real += a * c - b * e
            p_imag += a * e + b * c
        scale = hits_ref[d : d + 1]
        p_real *= scale
        p_imag *= scale
        for step in range(pieces):
            n = energies + ways * (here ^ step) + (role if step == 0 else 1 - role) - d
            a, b = g_ref[n, 0], g_ref[n, 1]
            totals[step][0] += a * p_real - b * p_imag
            totals[step][1] += a * p_imag + b * p_real
    weight = w_ref[...]
    for step in range(pieces):
        out_refs[step][0] = totals[step][0] * weight
        out_refs[step][1] = totals[step][1] * weight


def screen_kernel(offsets_ref, weight_ref, g_ref, out_ref):
    energies = g_ref.shape[0]
    count = offsets_ref.shape[0]
    factor = 6.0 / energies / (2.0 * 3.141592653589793) / count
    weight = weight_ref[...]

    def uses(offset):
        return lax.fori_loop(
            0, count, lambda i, total: total + jnp.where(offsets_ref[i] == offset, 1, 0), jnp.int32(0)
        )

    out_ref[...] = jnp.zeros_like(out_ref)

    @pl.loop(0, energies)
    def _(d):
        hits = uses(d)

        @pl.when(hits > 0)
        def _():
            scale = weight * (factor * hits.astype(F32))

            def gather(n, total):
                a, b, c, e = g_ref[n, 0], g_ref[n, 1], g_ref[n - d, 0], g_ref[n - d, 1]
                return total[0] + a * c - b * e, total[1] + a * e + b * c

            zero = jnp.zeros_like(weight)
            p_real, p_imag = lax.fori_loop(d, energies, gather, (zero, zero))
            p_real, p_imag = p_real * scale, p_imag * scale

            @pl.loop(d, energies)
            def _(n):
                a, b = g_ref[n - d, 0], g_ref[n - d, 1]
                out_ref[n, 0] += a * p_real - b * p_imag
                out_ref[n, 1] += a * p_imag + b * p_real


VM = pl.BlockSpec(memory_space=pltpu.VMEM)
SM = pl.BlockSpec(memory_space=pltpu.SMEM)
HB = pl.BlockSpec(memory_space=pltpu.HBM)
LIMIT = 8 * 2**20
PARAMS = pltpu.CompilerParams(vmem_limit_bytes=LIMIT)
MOST_STEPS = 8


def array(*shape):
    return jax.ShapeDtypeStruct(shape, F32)


def swap(value, axis, step):
    ways = lax.axis_size(axis)
    return lax.ppermute(value, axis, [(i, i ^ step) for i in range(ways)])


def exchange(values):
    ways, roles = lax.axis_size("energy"), lax.axis_size("role")
    result = list(values)
    for step in reversed(range(1, len(values))):
        pairs = [(i * roles + j, (i ^ step) * roles + 1 - j) for i in range(ways) for j in range(roles)]
        result[step] = lax.ppermute(values[step], ("energy", "role"), pairs)
    return result


def body(sigma_in, hamiltonian, coupling, coulomb, pattern, offsets):
    size = hamiltonian.shape[-1]
    blocks = lax.axis_size("block")
    ways_energy = lax.axis_size("energy")
    ways_role = lax.axis_size("role")
    groups = ways_energy * ways_role
    rows = size // groups
    assert blocks == 4 and sigma_in.shape[1] == 1 and ways_role == 2
    share = size // ways_role
    packed = pl.pallas_call(
        functools.partial(prepare_kernel, groups, blocks - 1),
        out_shape=array(2 * size + share, size),
        in_specs=[HB] * 4,
        out_specs=VM,
        scratch_shapes=[
            pltpu.SMEM(pattern.shape, jnp.int32),
            pltpu.VMEM((2, size, size), F32),
            pltpu.VMEM((size, size), F32),
            pltpu.VMEM((size, size), F32),
            pltpu.SemaphoreType.DMA((4,)),
        ],
        name="prepare",
        compiler_params=PARAMS,
    )(*(pltpu.with_memory_space_constraint(v, pltpu.HBM) for v in (pattern, sigma_in, hamiltonian, coupling)))
    weight = pl.pallas_call(
        weight_kernel,
        out_shape=array(rows, size),
        in_specs=[SM, VM],
        out_specs=VM,
        name="weight",
        compiler_params=PARAMS,
    )(pattern, coulomb.reshape(rows, size))
    gathered = lax.all_gather(packed, "block", axis=0, tiled=False)
    shares = pl.pallas_call(
        share_kernel,
        out_shape=array(blocks - 1, share, size),
        in_specs=[VM],
        out_specs=VM,
        name="share",
        compiler_params=PARAMS,
    )(gathered)
    partner = swap(shares, "role", 1)
    wide = (size, 2 * size)
    work = [
        pltpu.VMEM((2,) + wide, F32),
        pltpu.VMEM((2,) + wide, F32),
        pltpu.VMEM((2,) + wide, F32),
        pltpu.VMEM((2, 2, 2 * size, 2 * size), BF16),
    ]
    better, square = pl.pallas_call(
        side_kernel,
        out_shape=(array(2, *wide), array(2, *wide)),
        in_specs=[VM],
        out_specs=(VM, VM),
        scratch_shapes=work,
        name="side",
        compiler_params=PARAMS,
        cost_estimate=pl.CostEstimate(flops=2 * 10**9, bytes_accessed=2**20, transcendentals=0),
    )(gathered)
    direct = ways_energy <= MOST_STEPS
    pieces = ways_energy if direct else 1
    chunk = size // pieces
    parts = pl.pallas_call(
        functools.partial(green_kernel, pieces),
        out_shape=(array(2, chunk, size),) * pieces,
        in_specs=[VM] * 5,
        out_specs=(VM,) * pieces,
        scratch_shapes=work + [pltpu.VMEM((6, size, size), F32), pltpu.VMEM((2,) + wide, F32)],
        name="green",
        compiler_params=PARAMS,
    )(gathered, shares, partner, better, square)
    if not direct:
        green = parts[0].reshape(2, 1, 1, size, size)
        spread = lax.all_to_all(
            parts[0].reshape(2, groups, rows, size).transpose(1, 0, 2, 3),
            ("energy", "role"), split_axis=0, concat_axis=0, tiled=True,
        )
        screened = pl.pallas_call(
            screen_kernel,
            out_shape=array(*spread.shape),
            in_specs=[SM, VM, VM],
            out_specs=VM,
            name="screen",
        )(offsets, weight, spread)
        returned = lax.all_to_all(
            screened, ("energy", "role"), split_axis=0, concat_axis=0, tiled=True
        )
        return green, returned.transpose(1, 0, 2, 3).reshape(2, 1, 1, size, size)

    def join(name, values):
        return pl.pallas_call(
            join_kernel,
            out_shape=array(2, 1, 1, size, size),
            in_specs=[VM] * pieces,
            out_specs=HB,
            scratch_shapes=[pltpu.SemaphoreType.DMA((pieces,))],
            name=name,
            compiler_params=PARAMS,
        )(*values[::-1])

    arrived = exchange(parts)
    green = join("green_out", parts)
    own = pl.pallas_call(
        merge_kernel,
        out_shape=array(2 * chunk * pieces + rows, size),
        in_specs=[VM] * (pieces + 1),
        out_specs=VM,
        name="merge",
        compiler_params=PARAMS,
    )(weight, *arrived[::-1])
    other = swap(own, "role", 1)
    factor = 6.0 / groups / (2.0 * 3.141592653589793) / offsets.shape[0]
    hits = jnp.sum(offsets[None, :] == jnp.arange(groups)[:, None], axis=1, keepdims=True)
    hits = jnp.broadcast_to(factor * hits.astype(F32), (groups, size))
    screened = pl.pallas_call(
        pair_screen_kernel,
        out_shape=(array(2, chunk, size),) * pieces,
        in_specs=[VM, VM, VM],
        out_specs=(VM,) * pieces,
        scratch_shapes=[
            pltpu.VMEM((2 * groups, 2, chunk, size), F32),
            pltpu.VMEM((chunk, size), F32),
        ],
        name="screen",
        compiler_params=PARAMS,
    )(hits, own, other)
    return green, join("sigma_out", exchange(screened))


def solution(mesh):
    in_specs = (
        P(None, ("energy", "role"), "block", None, None),
        P("block", None, None),
        P("block", None, None),
        P("block", ("energy", "role")),
        P(None, "block", None, None),
        P(),
    )
    out_specs = (
        P(None, ("energy", "role"), "block", None, None),
        P(None, ("energy", "role"), "block", None, None),
    )
    return jax.shard_map(body, mesh=mesh, in_specs=in_specs, out_specs=out_specs, check_vma=False)
```

```python
import functools

import jax
import jax.numpy as jnp
from jax import lax
from jax.experimental import pallas as pl
from jax.experimental.pallas import tpu as pltpu
from jax.sharding import PartitionSpec as P

ETA = 0.1
CONTACT = 0.5
HIGH = lax.Precision.HIGHEST
F32 = jnp.float32
BF16 = jnp.bfloat16

LOW = 2.5e-4
STEPS = 7
TRUST = 2e-4
TOL = 1e-6
MAX_SAFE = 300


def step_table(low, steps):
    rows = []
    for _ in range(steps):
        scale = 4.0 / (1.0 + low) ** 2
        rows.append((scale * (1.0 + low), scale))
        low = scale * low
    return rows, 2.0 / (1.0 + low)


def split(value):
    high = value.astype(BF16)
    return high, (value - high.astype(F32)).astype(BF16)


def dot(left, right):
    return jnp.dot(left, right, preferred_element_type=F32)


def dot_turned(left, right):
    return lax.dot_general(left, right, (((1,), (1,)), ((), ())), preferred_element_type=F32)


def normal_matrix(parts, weights):
    return dot_turned(parts[0], weights[0]) + (
        dot_turned(parts[0], weights[1]) + dot_turned(parts[1], weights[0])
    )


def dot3(left, right):
    rows = left[0].shape[0]
    both = dot(jnp.concatenate([left[0], left[1]], axis=0), right[0])
    return (both[:rows] + both[rows:]) + dot(left[0], right[1])


def embed(wide):
    half = wide.shape[1] // 2
    return jnp.concatenate(
        [wide, jnp.concatenate([-wide[:, half:], wide[:, :half]], axis=1)], axis=0
    )


def embed_both(parts):
    return embed(parts[0]), embed(parts[1])


def wide_eye(size):
    row = lax.broadcasted_iota(jnp.int32, (size, 2 * size), 0)
    col = lax.broadcasted_iota(jnp.int32, (size, 2 * size), 1)
    return jnp.where(row == col, 1.0, 0.0).astype(F32)


def adjoint(wide):
    half = wide.shape[1] // 2
    return jnp.concatenate([wide[:, :half].T, -wide[:, half:].T], axis=1)


def rough_inverse(slots, s_ref, x_ref, t_ref, e_ref, beside=()):
    beside = list(beside)
    size = s_ref.shape[1]
    table, last = step_table(LOW, STEPS)
    for slot in slots:
        value = s_ref[slot]
        parts = split(value)
        weights = embed_both(parts)
        e_ref[slot, 0], e_ref[slot, 1] = weights
        t_ref[slot] = normal_matrix(parts, weights)
        x_ref[slot] = adjoint(value)
    for index in range(STEPS):
        lift, scale = table[index]
        for slot in slots:
            power = t_ref[slot]
            approx = x_ref[slot]
            parts = split(power)
            weights = embed_both(parts)
            if index == 0:
                alpha = inverse_bound(power)
                t_ref[slot] = (lift * alpha) * power - (scale * alpha * alpha) * dot3(parts, weights)
                x_ref[slot] = (lift * alpha) * approx - (scale * alpha * alpha) * dot3(
                    split(approx), weights
                )
            elif index < STEPS - 1:
                t_ref[slot] = lift * power - scale * dot3(parts, weights)
                x_ref[slot] = lift * approx - scale * dot3(split(approx), weights)
            else:
                x_ref[slot] = (last * lift) * approx - (last * scale) * dot(
                    approx.astype(BF16), weights[0]
                )
        if beside:
            beside.pop(0)()
    assert not beside


def inverse_bound(normal):
    size = normal.shape[0]
    sizes = jnp.sqrt(normal[:, :size] ** 2 + normal[:, size:] ** 2)
    bound = jnp.max(jnp.sum(sizes, axis=0, keepdims=True), axis=1, keepdims=True)
    return jnp.broadcast_to(1.0 / bound, (1, 2 * size))


def correction(slot, x_ref, e_ref):
    approx = x_ref[slot]
    parts = split(approx)
    rest = wide_eye(approx.shape[0]) - dot3(parts, (e_ref[slot, 0], e_ref[slot, 1]))
    rest_parts = split(rest)
    square = dot(rest_parts[0], embed(rest_parts[0]))
    better = approx + dot3(rest_parts, embed_both(parts))
    return better, square


def small(square):
    return jnp.sum(square * square) < TRUST


def safe_inverse(slot, s_ref, x_ref, e_ref):
    value = s_ref[slot]
    parts = split(value)
    weights = embed_both(parts)
    e_ref[slot, 0], e_ref[slot, 1] = weights
    x_ref[slot] = adjoint(value) * inverse_bound(normal_matrix(parts, weights))

    def unfinished(state):
        return jnp.logical_and(state[0] < MAX_SAFE, jnp.logical_not(state[1] < TOL))

    def refine(state):
        approx = x_ref[slot]
        parts = split(approx)
        rest = wide_eye(approx.shape[0]) - dot3(parts, (e_ref[slot, 0], e_ref[slot, 1]))
        x_ref[slot] = approx + dot3(split(rest), embed_both(parts))
        return state[0] + 1, jnp.sum(rest * rest)

    lax.while_loop(unfinished, refine, (jnp.int32(0), jnp.float32(1e30)))


def stack_parts(wide):
    half = wide.shape[1] // 2
    return jnp.concatenate([wide[:, :half], wide[:, half:]], axis=0)


def right_real(wide, matrix):
    rows = wide.shape[0]
    result = dot3(split(stack_parts(wide)), split(matrix))
    return jnp.concatenate([result[:rows], result[rows:]], axis=1)


def fetch(pairs, sems):
    copies = [pltpu.make_async_copy(source, target, sems.at[i]) for i, (source, target) in enumerate(pairs)]
    for copy in copies:
        copy.start()
    return copies


def tile_lines(pattern_ref, which, tile_row, size):
    tiles = pattern_ref.shape[-1]
    lane = lax.broadcasted_iota(jnp.int32, (1, size), 1) // (size // tiles)
    line = jnp.zeros((1, size), F32)
    for column in range(tiles):
        line = jnp.where(lane == column, pattern_ref[which, 0, tile_row, column].astype(F32), line)
    return line


def prepare_kernel(
    total, last_block, pattern_hbm, sigma_hbm, ham_hbm, coupling_hbm,
    out_ref, pattern_ref, sigma_ref, ham_ref, coupling_ref, sems,
):
    size = ham_ref.shape[-1]
    tiles = pattern_ref.shape[-1]
    tile = size // tiles
    copies = fetch(
        (
            (pattern_hbm, pattern_ref),
            (ham_hbm.at[0], ham_ref),
            (coupling_hbm.at[0], coupling_ref),
            (sigma_hbm.at[:, 0, 0], sigma_ref),
        ),
        sems,
    )
    block = lax.axis_index("block")
    role = lax.axis_index("role")
    place = lax.axis_index("energy") * lax.axis_size("role") + role
    row = lax.broadcasted_iota(jnp.int32, (size, size), 0)
    col = lax.broadcasted_iota(jnp.int32, (size, size), 1)
    number = jnp.full((size, size), place, jnp.int32).astype(F32)
    energy = jnp.where(row == col, -3.0 + 6.0 * number / total, 0.0)
    for copy in copies:
        copy.wait()
    mask = jnp.concatenate(
        [jnp.broadcast_to(tile_lines(pattern_ref, 0, t, size), (tile, size)) for t in range(tiles)],
        axis=0,
    )
    masked = ham_ref[...] * mask
    onsite = 0.5 * (masked + masked.T)
    out_ref[:size] = energy - onsite - sigma_ref[0]
    out_ref[size : 2 * size] = jnp.where(row == col, ETA, 0.0) - sigma_ref[1]
    share = out_ref.shape[0] - 2 * size
    out_ref[2 * size :] = coupling_ref[pl.ds(pl.multiple_of(role * share, share), share)]

    @pl.when(block == last_block)
    def _():
        square = dot3(split(coupling_ref[...].T), split(coupling_ref[...]))
        out_ref[size : 2 * size] += CONTACT * square


def weight_kernel(pattern_ref, coulomb_ref, weight_ref):
    rows, size = coulomb_ref.shape
    tile = size // pattern_ref.shape[-1]
    place = lax.axis_index("energy") * lax.axis_size("role") + lax.axis_index("role")
    for local_row in range(rows):
        line = tile_lines(pattern_ref, 1, (place * rows + local_row) // tile, size)
        value = coulomb_ref[local_row : local_row + 1] * line
        weight_ref[local_row : local_row + 1] = value * value


def share_kernel(all_ref, out_ref):
    first = all_ref.shape[1] - out_ref.shape[1]
    for block in range(out_ref.shape[0]):
        out_ref[block] = all_ref[block, first:]


def neighbours():
    own = lax.axis_index("block")
    low_half = own % 2 == 0
    return own, own ^ 2, jnp.where(low_half, 1, 2), jnp.where(low_half, 3, 0)


def wide_base(all_ref, block):
    size = all_ref.shape[-1]
    return jnp.concatenate([all_ref[block, :size], all_ref[block, size : 2 * size]], axis=1)


def side_kernel(all_ref, better_ref, square_ref, s_ref, x_ref, t_ref, e_ref):
    _, _, middle, other = neighbours()
    s_ref[0] = wide_base(all_ref, middle)
    s_ref[1] = wide_base(all_ref, other)
    rough_inverse((0, 1), s_ref, x_ref, t_ref, e_ref)
    for slot in range(2):
        better_ref[slot], square_ref[slot] = correction(slot, x_ref, e_ref)


def green_kernel(pieces, all_ref, mine_ref, theirs_ref, better_ref, square_ref, *refs):
    out_refs, (s_ref, x_ref, t_ref, e_ref, k_ref, up_ref, r_ref) = refs[:-7], refs[-7:]
    size = all_ref.shape[-1]
    own, far, middle, other = neighbours()
    role = lax.axis_index("role")

    def base(block):
        return wide_base(all_ref, block)

    share = mine_ref.shape[1]
    for block in range(3):
        for index, ref in ((role, mine_ref), (1 - role, theirs_ref)):
            k_ref[block, pl.ds(pl.multiple_of(index * share, share), share)] = ref[block]
        k_ref[3 + block] = k_ref[block].T

    def link(source, target):
        return k_ref[jnp.where(target > source, source, 3 + target)]

    beside = jnp.where(own % 2 == 0, 2, 1)
    beside_far = beside == far

    def reduce(better, square):
        def left(matrix, slot):
            first = dot(matrix.astype(BF16), square[slot].astype(BF16))
            return jnp.concatenate([matrix + first[:, :size], first[:, size:]], axis=1)

        def product(first, second):
            return dot3(split(first), embed_both(split(second)))

        far_left = left(link(far, middle), 0)
        far_right = right_real(better[0], link(middle, far))
        side = product(left(link(beside, other), 1), right_real(better[1], link(other, beside)))
        s_ref[0] = base(far) - product(far_left, far_right) - jnp.where(beside_far, side, 0.0)
        s_ref[1] = base(own) - jnp.where(beside_far, 0.0, side)
        up_ref[0] = far_left
        up_ref[1] = far_right

        def prepare_own():
            r_ref[0] = left(link(own, middle), 0)
            r_ref[1] = right_real(better[0], link(middle, own))

        def own_system():
            s_ref[1] -= product(r_ref[0], r_ref[1])

        def coupling_up():
            r_ref[2] = product(r_ref[0], up_ref[1])

        def coupling_down():
            up_ref[1] = product(up_ref[0], r_ref[1])
            up_ref[0] = r_ref[2]

        return prepare_own, own_system, coupling_up, coupling_down

    work = reduce((better_ref[0], better_ref[1]), (square_ref[0], square_ref[1]))
    good = jnp.logical_and(small(square_ref[0]), small(square_ref[1]))

    rough_inverse((0,), s_ref, x_ref, t_ref, e_ref, work)
    better, square = correction(0, x_ref, e_ref)
    good = jnp.logical_and(good, small(square))
    up = up_ref[0]
    left = up + dot(up.astype(BF16), embed(square.astype(BF16)))
    right = dot3(split(better), embed_both(split(up_ref[1])))
    s_ref[0] = s_ref[1] - dot3(split(left), embed_both(split(right)))

    rough_inverse((0,), s_ref, x_ref, t_ref, e_ref)
    better, square = correction(0, x_ref, e_ref)
    good = jnp.logical_and(good, small(square))
    x_ref[0] = better + dot(square.astype(BF16), embed(better.astype(BF16)))

    @pl.when(jnp.logical_not(good))
    def _():
        s_ref[0] = base(middle)
        safe_inverse(0, s_ref, x_ref, e_ref)
        s_ref[1] = base(other)
        safe_inverse(1, s_ref, x_ref, e_ref)
        zero = jnp.zeros((size, 2 * size), F32)
        for step in reduce((x_ref[0], x_ref[1]), (zero, zero)):
            step()
        safe_inverse(0, s_ref, x_ref, e_ref)
        first = dot3(split(up_ref[0]), embed_both(split(x_ref[0])))
        s_ref[0] = s_ref[1] - dot3(split(first), embed_both(split(up_ref[1])))
        safe_inverse(0, s_ref, x_ref, e_ref)

    if pieces == 1:
        out_refs[0][0] = x_ref[0, :, :size]
        out_refs[0][1] = x_ref[0, :, size:]
        return
    rows = size // pieces
    here = lax.axis_index("energy")
    for step in range(pieces):
        part = pl.ds(pl.multiple_of((here ^ step) * rows, rows), rows)
        out_refs[step][0] = x_ref[0, part, :size]
        out_refs[step][1] = x_ref[0, part, size:]


def join_kernel(*refs):
    out_hbm, sems = refs[-2:]
    pieces = len(refs) - 2
    rows = refs[0].shape[1]
    here = lax.axis_index("energy")
    copies = fetch(
        [
            (refs[pieces - 1 - step], out_hbm.at[:, 0, 0, pl.ds(pl.multiple_of((here ^ step) * rows, rows), rows)])
            for step in range(pieces)
        ],
        sems,
    )
    for copy in copies:
        copy.wait()


def merge_kernel(weight_ref, *refs):
    out_ref = refs[-1]
    rows = refs[0].shape[1]
    for step, ref in enumerate(refs[:-1][::-1]):
        for part in range(2):
            start = (2 * step + part) * rows
            out_ref[start : start + rows] = ref[part]
    start = 2 * rows * (len(refs) - 1)
    out_ref[start : start + weight_ref.shape[0]] = weight_ref[...]


def pair_screen_kernel(hits_ref, own_ref, other_ref, *refs):
    out_refs, (g_ref, w_ref) = refs[:-2], refs[-2:]
    pieces = len(out_refs)
    energies = g_ref.shape[0] // 2
    rows = g_ref.shape[2]
    ways = energies // pieces
    here = lax.axis_index("energy")
    role = lax.axis_index("role")
    g_ref[:energies] = jnp.zeros((energies, 2) + g_ref.shape[2:], F32)
    half = w_ref.shape[0] // ways
    start = 2 * rows * pieces
    for index, ref in ((role, own_ref), (1 - role, other_ref)):
        for step in range(pieces):
            n = energies + ways * (here ^ step) + (index if step == 0 else 1 - index)
            for part in range(2):
                first = (2 * step + part) * rows
                g_ref[n, part] = ref[first : first + rows]
        w_ref[pl.ds(pl.multiple_of(index * half, half), half)] = ref[start : start + half]
    totals = [[jnp.zeros(g_ref.shape[2:], F32) for _ in range(2)] for _ in range(pieces)]
    for d in range(energies):
        p_real = jnp.zeros(g_ref.shape[2:], F32)
        p_imag = jnp.zeros(g_ref.shape[2:], F32)
        for n in range(d, energies):
            a, b = g_ref[energies + n, 0], g_ref[energies + n, 1]
            c, e = g_ref[energies + n - d, 0], g_ref[energies + n - d, 1]
            p_real += a * c - b * e
            p_imag += a * e + b * c
        scale = hits_ref[d : d + 1]
        p_real *= scale
        p_imag *= scale
        for step in range(pieces):
            n = energies + ways * (here ^ step) + (role if step == 0 else 1 - role) - d
            a, b = g_ref[n, 0], g_ref[n, 1]
            totals[step][0] += a * p_real - b * p_imag
            totals[step][1] += a * p_imag + b * p_real
    weight = w_ref[...]
    for step in range(pieces):
        out_refs[step][0] = totals[step][0] * weight
        out_refs[step][1] = totals[step][1] * weight


def screen_kernel(offsets_ref, weight_ref, g_ref, out_ref):
    energies = g_ref.shape[0]
    count = offsets_ref.shape[0]
    factor = 6.0 / energies / (2.0 * 3.141592653589793) / count
    weight = weight_ref[...]

    def uses(offset):
        return lax.fori_loop(
            0, count, lambda i, total: total + jnp.where(offsets_ref[i] == offset, 1, 0), jnp.int32(0)
        )

    out_ref[...] = jnp.zeros_like(out_ref)

    @pl.loop(0, energies)
    def _(d):
        hits = uses(d)

        @pl.when(hits > 0)
        def _():
            scale = weight * (factor * hits.astype(F32))

            def gather(n, total):
                a, b, c, e = g_ref[n, 0], g_ref[n, 1], g_ref[n - d, 0], g_ref[n - d, 1]
                return total[0] + a * c - b * e, total[1] + a * e + b * c

            zero = jnp.zeros_like(weight)
            p_real, p_imag = lax.fori_loop(d, energies, gather, (zero, zero))
            p_real, p_imag = p_real * scale, p_imag * scale

            @pl.loop(d, energies)
            def _(n):
                a, b = g_ref[n - d, 0], g_ref[n - d, 1]
                out_ref[n, 0] += a * p_real - b * p_imag
                out_ref[n, 1] += a * p_imag + b * p_real


VM = pl.BlockSpec(memory_space=pltpu.VMEM)
SM = pl.BlockSpec(memory_space=pltpu.SMEM)
HB = pl.BlockSpec(memory_space=pltpu.HBM)
LIMIT = 8 * 2**20
PARAMS = pltpu.CompilerParams(vmem_limit_bytes=LIMIT)
MOST_STEPS = 8


def array(*shape):
    return jax.ShapeDtypeStruct(shape, F32)


def swap(value, axis, step):
    ways = lax.axis_size(axis)
    return lax.ppermute(value, axis, [(i, i ^ step) for i in range(ways)])


def exchange(values):
    ways, roles = lax.axis_size("energy"), lax.axis_size("role")
    result = list(values)
    for step in reversed(range(1, len(values))):
        pairs = [(i * roles + j, (i ^ step) * roles + 1 - j) for i in range(ways) for j in range(roles)]
        result[step] = lax.ppermute(values[step], ("energy", "role"), pairs)
    return result


def body(sigma_in, hamiltonian, coupling, coulomb, pattern, offsets):
    size = hamiltonian.shape[-1]
    blocks = lax.axis_size("block")
    ways_energy = lax.axis_size("energy")
    ways_role = lax.axis_size("role")
    groups = ways_energy * ways_role
    rows = size // groups
    assert blocks == 4 and sigma_in.shape[1] == 1 and ways_role == 2
    share = size // ways_role
    packed = pl.pallas_call(
        functools.partial(prepare_kernel, groups, blocks - 1),
        out_shape=array(2 * size + share, size),
        in_specs=[HB] * 4,
        out_specs=VM,
        scratch_shapes=[
            pltpu.SMEM(pattern.shape, jnp.int32),
            pltpu.VMEM((2, size, size), F32),
            pltpu.VMEM((size, size), F32),
            pltpu.VMEM((size, size), F32),
            pltpu.SemaphoreType.DMA((4,)),
        ],
        name="prepare",
        compiler_params=PARAMS,
    )(*(pltpu.with_memory_space_constraint(v, pltpu.HBM) for v in (pattern, sigma_in, hamiltonian, coupling)))
    weight = pl.pallas_call(
        weight_kernel,
        out_shape=array(rows, size),
        in_specs=[SM, VM],
        out_specs=VM,
        name="weight",
        compiler_params=PARAMS,
    )(pattern, coulomb.reshape(rows, size))
    gathered = lax.all_gather(packed, "block", axis=0, tiled=False)
    shares = pl.pallas_call(
        share_kernel,
        out_shape=array(blocks - 1, share, size),
        in_specs=[VM],
        out_specs=VM,
        name="share",
        compiler_params=PARAMS,
    )(gathered)
    partner = swap(shares, "role", 1)
    wide = (size, 2 * size)
    work = [
        pltpu.VMEM((2,) + wide, F32),
        pltpu.VMEM((2,) + wide, F32),
        pltpu.VMEM((2,) + wide, F32),
        pltpu.VMEM((2, 2, 2 * size, 2 * size), BF16),
    ]
    better, square = pl.pallas_call(
        side_kernel,
        out_shape=(array(2, *wide), array(2, *wide)),
        in_specs=[VM],
        out_specs=(VM, VM),
        scratch_shapes=work,
        name="side",
        compiler_params=PARAMS,
        cost_estimate=pl.CostEstimate(flops=2 * 10**9, bytes_accessed=2**20, transcendentals=0),
    )(gathered)
    direct = ways_energy <= MOST_STEPS
    pieces = ways_energy if direct else 1
    chunk = size // pieces
    parts = pl.pallas_call(
        functools.partial(green_kernel, pieces),
        out_shape=(array(2, chunk, size),) * pieces,
        in_specs=[VM] * 5,
        out_specs=(VM,) * pieces,
        scratch_shapes=work + [pltpu.VMEM((6, size, size), F32), pltpu.VMEM((2,) + wide, F32), pltpu.VMEM((3,) + wide, F32)],
        name="green",
        compiler_params=PARAMS,
    )(gathered, shares, partner, better, square)
    if not direct:
        green = parts[0].reshape(2, 1, 1, size, size)
        spread = lax.all_to_all(
            parts[0].reshape(2, groups, rows, size).transpose(1, 0, 2, 3),
            ("energy", "role"), split_axis=0, concat_axis=0, tiled=True,
        )
        screened = pl.pallas_call(
            screen_kernel,
            out_shape=array(*spread.shape),
            in_specs=[SM, VM, VM],
            out_specs=VM,
            name="screen",
        )(offsets, weight, spread)
        returned = lax.all_to_all(
            screened, ("energy", "role"), split_axis=0, concat_axis=0, tiled=True
        )
        return green, returned.transpose(1, 0, 2, 3).reshape(2, 1, 1, size, size)

    def join(name, values):
        return pl.pallas_call(
            join_kernel,
            out_shape=array(2, 1, 1, size, size),
            in_specs=[VM] * pieces,
            out_specs=HB,
            scratch_shapes=[pltpu.SemaphoreType.DMA((pieces,))],
            name=name,
            compiler_params=PARAMS,
        )(*values[::-1])

    arrived = exchange(parts)
    green = join("green_out", parts)
    own = pl.pallas_call(
        merge_kernel,
        out_shape=array(2 * chunk * pieces + rows, size),
        in_specs=[VM] * (pieces + 1),
        out_specs=VM,
        name="merge",
        compiler_params=PARAMS,
    )(weight, *arrived[::-1])
    other = swap(own, "role", 1)
    factor = 6.0 / groups / (2.0 * 3.141592653589793) / offsets.shape[0]
    hits = jnp.sum(offsets[None, :] == jnp.arange(groups)[:, None], axis=1, keepdims=True)
    hits = jnp.broadcast_to(factor * hits.astype(F32), (groups, size))
    screened = pl.pallas_call(
        pair_screen_kernel,
        out_shape=(array(2, chunk, size),) * pieces,
        in_specs=[VM, VM, VM],
        out_specs=(VM,) * pieces,
        scratch_shapes=[
            pltpu.VMEM((2 * groups, 2, chunk, size), F32),
            pltpu.VMEM((chunk, size), F32),
        ],
        name="screen",
        compiler_params=PARAMS,
    )(hits, own, other)
    return green, join("sigma_out", exchange(screened))


def solution(mesh):
    in_specs = (
        P(None, ("energy", "role"), "block", None, None),
        P("block", None, None),
        P("block", None, None),
        P("block", ("energy", "role")),
        P(None, "block", None, None),
        P(),
    )
    out_specs = (
        P(None, ("energy", "role"), "block", None, None),
        P(None, ("energy", "role"), "block", None, None),
    )
    return jax.shard_map(body, mesh=mesh, in_specs=in_specs, out_specs=out_specs, check_vma=False)
```

```python
import functools

import jax
import jax.numpy as jnp
from jax import lax
from jax.experimental import pallas as pl
from jax.experimental.pallas import tpu as pltpu
from jax.sharding import PartitionSpec as P

ETA = 0.1
CONTACT = 0.5
F32 = jnp.float32
BF16 = jnp.bfloat16

LOW = 2.5e-4
HEAD = 1.6
STEPS = 7
TRUST = 2e-4
TOL = 1e-6
MAX_SAFE = 300


def step_table(low, steps):
    rows = []
    for _ in range(steps):
        scale = 4.0 / (1.0 + low) ** 2
        rows.append((scale * (1.0 + low), scale))
        low = scale * low
    return rows, 2.0 / (1.0 + low)


def split(value):
    high = value.astype(BF16)
    return high, (value - high.astype(F32)).astype(BF16)


def dot(left, right):
    return jnp.dot(left, right, preferred_element_type=F32)


def dot_turned(left, right):
    return lax.dot_general(left, right, (((1,), (1,)), ((), ())), preferred_element_type=F32)


def normal_matrix(parts, weights):
    return dot_turned(parts[0], weights[0]) + (
        dot_turned(parts[0], weights[1]) + dot_turned(parts[1], weights[0])
    )


def dot3(left, right):
    rows = left[0].shape[0]
    both = dot(jnp.concatenate([left[0], left[1]], axis=0), right[0])
    return (both[:rows] + both[rows:]) + dot(left[0], right[1])


def embed(wide):
    half = wide.shape[1] // 2
    return jnp.concatenate(
        [wide, jnp.concatenate([-wide[:, half:], wide[:, :half]], axis=1)], axis=0
    )


def embed_both(parts):
    return embed(parts[0]), embed(parts[1])


def wide_eye(size):
    row = lax.broadcasted_iota(jnp.int32, (size, 2 * size), 0)
    col = lax.broadcasted_iota(jnp.int32, (size, 2 * size), 1)
    return jnp.where(row == col, 1.0, 0.0).astype(F32)


def adjoint(wide):
    half = wide.shape[1] // 2
    return jnp.concatenate([wide[:, :half].T, -wide[:, half:].T], axis=1)


def rough_inverse(slots, s_ref, x_ref, t_ref, e_ref, beside=()):
    beside = list(beside)
    size = s_ref.shape[1]
    table, last = step_table(LOW, STEPS)
    for slot in slots:
        value = s_ref[slot]
        parts = split(value)
        weights = embed_both(parts)
        e_ref[slot, 0], e_ref[slot, 1] = weights
        t_ref[slot] = normal_matrix(parts, weights)
        x_ref[slot] = adjoint(value)
    for index in range(STEPS):
        lift, scale = table[index]
        for slot in slots:
            power = t_ref[slot]
            approx = x_ref[slot]
            parts = split(power)
            weights = embed_both(parts)
            if index == 0:
                alpha = HEAD * inverse_bound(power)
                t_ref[slot] = (lift * alpha) * power - (scale * alpha * alpha) * dot3(parts, weights)
                x_ref[slot] = (lift * alpha) * approx - (scale * alpha * alpha) * dot3(
                    split(approx), weights
                )
            elif index < STEPS - 1:
                t_ref[slot] = lift * power - scale * dot3(parts, weights)
                x_ref[slot] = lift * approx - scale * dot3(split(approx), weights)
            else:
                x_ref[slot] = (last * lift) * approx - (last * scale) * dot(
                    approx.astype(BF16), weights[0]
                )
        if beside:
            beside.pop(0)()
    assert not beside


def inverse_bound(normal):
    size = normal.shape[0]
    sizes = jnp.sqrt(normal[:, :size] ** 2 + normal[:, size:] ** 2)
    bound = jnp.max(jnp.sum(sizes, axis=0, keepdims=True), axis=1, keepdims=True)
    return jnp.broadcast_to(1.0 / bound, (1, 2 * size))


def correction(slot, x_ref, e_ref):
    approx = x_ref[slot]
    parts = split(approx)
    rest = wide_eye(approx.shape[0]) - dot3(parts, (e_ref[slot, 0], e_ref[slot, 1]))
    rest_parts = split(rest)
    square = dot(rest_parts[0], embed(rest_parts[0]))
    better = approx + dot3(rest_parts, embed_both(parts))
    return better, square


def small(square):
    return jnp.sum(square * square) < TRUST


def safe_inverse(slot, s_ref, x_ref, e_ref):
    value = s_ref[slot]
    parts = split(value)
    weights = embed_both(parts)
    e_ref[slot, 0], e_ref[slot, 1] = weights
    x_ref[slot] = adjoint(value) * inverse_bound(normal_matrix(parts, weights))

    def unfinished(state):
        return jnp.logical_and(state[0] < MAX_SAFE, jnp.logical_not(state[1] < TOL))

    def refine(state):
        approx = x_ref[slot]
        parts = split(approx)
        rest = wide_eye(approx.shape[0]) - dot3(parts, (e_ref[slot, 0], e_ref[slot, 1]))
        x_ref[slot] = approx + dot3(split(rest), embed_both(parts))
        return state[0] + 1, jnp.sum(rest * rest)

    lax.while_loop(unfinished, refine, (jnp.int32(0), jnp.float32(1e30)))


def stack_parts(wide):
    half = wide.shape[1] // 2
    return jnp.concatenate([wide[:, :half], wide[:, half:]], axis=0)


def right_real(wide, matrix):
    rows = wide.shape[0]
    result = dot3(split(stack_parts(wide)), split(matrix))
    return jnp.concatenate([result[:rows], result[rows:]], axis=1)


def fetch(pairs, sems):
    copies = [pltpu.make_async_copy(source, target, sems.at[i]) for i, (source, target) in enumerate(pairs)]
    for copy in copies:
        copy.start()
    return copies


def tile_lines(pattern_ref, which, tile_row, size):
    tiles = pattern_ref.shape[-1]
    lane = lax.broadcasted_iota(jnp.int32, (1, size), 1) // (size // tiles)
    line = jnp.zeros((1, size), F32)
    for column in range(tiles):
        line = jnp.where(lane == column, pattern_ref[which, 0, tile_row, column].astype(F32), line)
    return line


def prepare_kernel(
    total, last_block, pattern_hbm, sigma_hbm, ham_hbm, coupling_hbm,
    out_ref, pattern_ref, sigma_ref, ham_ref, coupling_ref, sems,
):
    size = ham_ref.shape[-1]
    tiles = pattern_ref.shape[-1]
    tile = size // tiles
    copies = fetch(
        (
            (pattern_hbm, pattern_ref),
            (ham_hbm.at[0], ham_ref),
            (coupling_hbm.at[0], coupling_ref),
            (sigma_hbm.at[:, 0, 0], sigma_ref),
        ),
        sems,
    )
    block = lax.axis_index("block")
    role = lax.axis_index("role")
    place = lax.axis_index("energy") * lax.axis_size("role") + role
    row = lax.broadcasted_iota(jnp.int32, (size, size), 0)
    col = lax.broadcasted_iota(jnp.int32, (size, size), 1)
    number = jnp.full((size, size), place, jnp.int32).astype(F32)
    energy = jnp.where(row == col, -3.0 + 6.0 * number / total, 0.0)
    for copy in copies:
        copy.wait()
    mask = jnp.concatenate(
        [jnp.broadcast_to(tile_lines(pattern_ref, 0, t, size), (tile, size)) for t in range(tiles)],
        axis=0,
    )
    masked = ham_ref[...] * mask
    onsite = 0.5 * (masked + masked.T)
    out_ref[:size] = energy - onsite - sigma_ref[0]
    out_ref[size : 2 * size] = jnp.where(row == col, ETA, 0.0) - sigma_ref[1]
    share = out_ref.shape[0] - 2 * size
    out_ref[2 * size :] = coupling_ref[pl.ds(pl.multiple_of(role * share, share), share)]

    @pl.when(block == last_block)
    def _():
        square = dot3(split(coupling_ref[...].T), split(coupling_ref[...]))
        out_ref[size : 2 * size] += CONTACT * square


def weight_kernel(pattern_ref, coulomb_ref, weight_ref):
    rows, size = coulomb_ref.shape
    tile = size // pattern_ref.shape[-1]
    place = lax.axis_index("energy") * lax.axis_size("role") + lax.axis_index("role")
    for local_row in range(rows):
        line = tile_lines(pattern_ref, 1, (place * rows + local_row) // tile, size)
        value = coulomb_ref[local_row : local_row + 1] * line
        weight_ref[local_row : local_row + 1] = value * value


def share_kernel(all_ref, out_ref):
    first = all_ref.shape[1] - out_ref.shape[1]
    for block in range(out_ref.shape[0]):
        out_ref[block] = all_ref[block, first:]


def neighbours():
    own = lax.axis_index("block")
    low_half = own % 2 == 0
    return own, own ^ 2, jnp.where(low_half, 1, 2), jnp.where(low_half, 3, 0)


def wide_base(all_ref, block):
    size = all_ref.shape[-1]
    return jnp.concatenate([all_ref[block, :size], all_ref[block, size : 2 * size]], axis=1)


def side_kernel(all_ref, better_ref, square_ref, s_ref, x_ref, t_ref, e_ref):
    _, _, middle, other = neighbours()
    s_ref[0] = wide_base(all_ref, middle)
    s_ref[1] = wide_base(all_ref, other)
    rough_inverse((0, 1), s_ref, x_ref, t_ref, e_ref)
    for slot in range(2):
        better_ref[slot], square_ref[slot] = correction(slot, x_ref, e_ref)


def green_kernel(pieces, all_ref, mine_ref, theirs_ref, better_ref, square_ref, *refs):
    out_refs, (s_ref, x_ref, t_ref, e_ref, k_ref, up_ref, r_ref) = refs[:-7], refs[-7:]
    size = all_ref.shape[-1]
    own, far, middle, other = neighbours()
    role = lax.axis_index("role")

    def base(block):
        return wide_base(all_ref, block)

    share = mine_ref.shape[1]
    for block in range(3):
        for index, ref in ((role, mine_ref), (1 - role, theirs_ref)):
            k_ref[block, pl.ds(pl.multiple_of(index * share, share), share)] = ref[block]
        k_ref[3 + block] = k_ref[block].T

    def link(source, target):
        return k_ref[jnp.where(target > source, source, 3 + target)]

    beside = jnp.where(own % 2 == 0, 2, 1)
    beside_far = beside == far

    def reduce(better, square):
        def left(matrix, slot):
            first = dot(matrix.astype(BF16), square[slot].astype(BF16))
            return jnp.concatenate([matrix + first[:, :size], first[:, size:]], axis=1)

        def product(first, second):
            return dot3(split(first), embed_both(split(second)))

        far_left = left(link(far, middle), 0)
        far_right = right_real(better[0], link(middle, far))
        side = product(left(link(beside, other), 1), right_real(better[1], link(other, beside)))
        s_ref[0] = base(far) - product(far_left, far_right) - jnp.where(beside_far, side, 0.0)
        s_ref[1] = base(own) - jnp.where(beside_far, 0.0, side)
        up_ref[0] = far_left
        up_ref[1] = far_right

        def prepare_own():
            r_ref[0] = left(link(own, middle), 0)
            r_ref[1] = right_real(better[0], link(middle, own))

        def own_system():
            s_ref[1] -= product(r_ref[0], r_ref[1])

        def coupling_up():
            r_ref[2] = product(r_ref[0], up_ref[1])

        def coupling_down():
            up_ref[1] = product(up_ref[0], r_ref[1])
            up_ref[0] = r_ref[2]

        return prepare_own, own_system, coupling_up, coupling_down

    work = reduce((better_ref[0], better_ref[1]), (square_ref[0], square_ref[1]))
    good = jnp.logical_and(small(square_ref[0]), small(square_ref[1]))

    rough_inverse((0,), s_ref, x_ref, t_ref, e_ref, work)
    better, square = correction(0, x_ref, e_ref)
    good = jnp.logical_and(good, small(square))
    up = up_ref[0]
    left = up + dot(up.astype(BF16), embed(square.astype(BF16)))
    right = dot3(split(better), embed_both(split(up_ref[1])))
    s_ref[0] = s_ref[1] - dot3(split(left), embed_both(split(right)))

    rough_inverse((0,), s_ref, x_ref, t_ref, e_ref)
    better, square = correction(0, x_ref, e_ref)
    good = jnp.logical_and(good, small(square))
    x_ref[0] = better + dot(square.astype(BF16), embed(better.astype(BF16)))

    @pl.when(jnp.logical_not(good))
    def _():
        s_ref[0] = base(middle)
        safe_inverse(0, s_ref, x_ref, e_ref)
        s_ref[1] = base(other)
        safe_inverse(1, s_ref, x_ref, e_ref)
        zero = jnp.zeros((size, 2 * size), F32)
        for step in reduce((x_ref[0], x_ref[1]), (zero, zero)):
            step()
        safe_inverse(0, s_ref, x_ref, e_ref)
        first = dot3(split(up_ref[0]), embed_both(split(x_ref[0])))
        s_ref[0] = s_ref[1] - dot3(split(first), embed_both(split(up_ref[1])))
        safe_inverse(0, s_ref, x_ref, e_ref)

    if pieces == 1:
        out_refs[0][0] = x_ref[0, :, :size]
        out_refs[0][1] = x_ref[0, :, size:]
        return
    rows = size // pieces
    here = lax.axis_index("energy")
    for step in range(pieces):
        part = pl.ds(pl.multiple_of((here ^ step) * rows, rows), rows)
        out_refs[step][0] = x_ref[0, part, :size]
        out_refs[step][1] = x_ref[0, part, size:]


def join_kernel(*refs):
    out_hbm, sems = refs[-2:]
    pieces = len(refs) - 2
    rows = refs[0].shape[1]
    here = lax.axis_index("energy")
    copies = fetch(
        [
            (refs[pieces - 1 - step], out_hbm.at[:, 0, 0, pl.ds(pl.multiple_of((here ^ step) * rows, rows), rows)])
            for step in range(pieces)
        ],
        sems,
    )
    for copy in copies:
        copy.wait()


def merge_kernel(weight_ref, *refs):
    out_ref = refs[-1]
    rows = refs[0].shape[1]
    for step, ref in enumerate(refs[:-1][::-1]):
        for part in range(2):
            start = (2 * step + part) * rows
            out_ref[start : start + rows] = ref[part]
    start = 2 * rows * (len(refs) - 1)
    out_ref[start : start + weight_ref.shape[0]] = weight_ref[...]


def pair_screen_kernel(hits_ref, own_ref, other_ref, *refs):
    out_refs, (g_ref, w_ref) = refs[:-2], refs[-2:]
    pieces = len(out_refs)
    energies = g_ref.shape[0] // 2
    rows = g_ref.shape[2]
    ways = energies // pieces
    here = lax.axis_index("energy")
    role = lax.axis_index("role")
    g_ref[:energies] = jnp.zeros((energies, 2) + g_ref.shape[2:], F32)
    half = w_ref.shape[0] // ways
    start = 2 * rows * pieces
    for index, ref in ((role, own_ref), (1 - role, other_ref)):
        for step in range(pieces):
            n = energies + ways * (here ^ step) + (index if step == 0 else 1 - index)
            for part in range(2):
                first = (2 * step + part) * rows
                g_ref[n, part] = ref[first : first + rows]
        w_ref[pl.ds(pl.multiple_of(index * half, half), half)] = ref[start : start + half]
    totals = [[jnp.zeros(g_ref.shape[2:], F32) for _ in range(2)] for _ in range(pieces)]
    for d in range(energies):
        p_real = jnp.zeros(g_ref.shape[2:], F32)
        p_imag = jnp.zeros(g_ref.shape[2:], F32)
        for n in range(d, energies):
            a, b = g_ref[energies + n, 0], g_ref[energies + n, 1]
            c, e = g_ref[energies + n - d, 0], g_ref[energies + n - d, 1]
            p_real += a * c - b * e
            p_imag += a * e + b * c
        scale = hits_ref[d : d + 1]
        p_real *= scale
        p_imag *= scale
        for step in range(pieces):
            n = energies + ways * (here ^ step) + (role if step == 0 else 1 - role) - d
            a, b = g_ref[n, 0], g_ref[n, 1]
            totals[step][0] += a * p_real - b * p_imag
            totals[step][1] += a * p_imag + b * p_real
    weight = w_ref[...]
    for step in range(pieces):
        out_refs[step][0] = totals[step][0] * weight
        out_refs[step][1] = totals[step][1] * weight


def screen_kernel(offsets_ref, weight_ref, g_ref, out_ref):
    energies = g_ref.shape[0]
    count = offsets_ref.shape[0]
    factor = 6.0 / energies / (2.0 * 3.141592653589793) / count
    weight = weight_ref[...]

    def uses(offset):
        return lax.fori_loop(
            0, count, lambda i, total: total + jnp.where(offsets_ref[i] == offset, 1, 0), jnp.int32(0)
        )

    out_ref[...] = jnp.zeros_like(out_ref)

    @pl.loop(0, energies)
    def _(d):
        hits = uses(d)

        @pl.when(hits > 0)
        def _():
            scale = weight * (factor * hits.astype(F32))

            def gather(n, total):
                a, b, c, e = g_ref[n, 0], g_ref[n, 1], g_ref[n - d, 0], g_ref[n - d, 1]
                return total[0] + a * c - b * e, total[1] + a * e + b * c

            zero = jnp.zeros_like(weight)
            p_real, p_imag = lax.fori_loop(d, energies, gather, (zero, zero))
            p_real, p_imag = p_real * scale, p_imag * scale

            @pl.loop(d, energies)
            def _(n):
                a, b = g_ref[n - d, 0], g_ref[n - d, 1]
                out_ref[n, 0] += a * p_real - b * p_imag
                out_ref[n, 1] += a * p_imag + b * p_real


VM = pl.BlockSpec(memory_space=pltpu.VMEM)
SM = pl.BlockSpec(memory_space=pltpu.SMEM)
HB = pl.BlockSpec(memory_space=pltpu.HBM)
LIMIT = 8 * 2**20
PARAMS = pltpu.CompilerParams(vmem_limit_bytes=LIMIT)
MOST_STEPS = 8


def array(*shape):
    return jax.ShapeDtypeStruct(shape, F32)


def swap(value, axis, step):
    ways = lax.axis_size(axis)
    return lax.ppermute(value, axis, [(i, i ^ step) for i in range(ways)])


def exchange(values):
    ways, roles = lax.axis_size("energy"), lax.axis_size("role")
    result = list(values)
    for step in reversed(range(1, len(values))):
        pairs = [(i * roles + j, (i ^ step) * roles + 1 - j) for i in range(ways) for j in range(roles)]
        result[step] = lax.ppermute(values[step], ("energy", "role"), pairs)
    return result


def body(sigma_in, hamiltonian, coupling, coulomb, pattern, offsets):
    size = hamiltonian.shape[-1]
    blocks = lax.axis_size("block")
    ways_energy = lax.axis_size("energy")
    ways_role = lax.axis_size("role")
    groups = ways_energy * ways_role
    rows = size // groups
    assert blocks == 4 and sigma_in.shape[1] == 1 and ways_role == 2
    share = size // ways_role
    packed = pl.pallas_call(
        functools.partial(prepare_kernel, groups, blocks - 1),
        out_shape=array(2 * size + share, size),
        in_specs=[HB] * 4,
        out_specs=VM,
        scratch_shapes=[
            pltpu.SMEM(pattern.shape, jnp.int32),
            pltpu.VMEM((2, size, size), F32),
            pltpu.VMEM((size, size), F32),
            pltpu.VMEM((size, size), F32),
            pltpu.SemaphoreType.DMA((4,)),
        ],
        name="prepare",
        compiler_params=PARAMS,
    )(*(pltpu.with_memory_space_constraint(v, pltpu.HBM) for v in (pattern, sigma_in, hamiltonian, coupling)))
    weight = pl.pallas_call(
        weight_kernel,
        out_shape=array(rows, size),
        in_specs=[SM, VM],
        out_specs=VM,
        name="weight",
        compiler_params=PARAMS,
    )(pattern, coulomb.reshape(rows, size))
    gathered = lax.all_gather(packed, "block", axis=0, tiled=False)
    shares = pl.pallas_call(
        share_kernel,
        out_shape=array(blocks - 1, share, size),
        in_specs=[VM],
        out_specs=VM,
        name="share",
        compiler_params=PARAMS,
    )(gathered)
    partner = swap(shares, "role", 1)
    wide = (size, 2 * size)
    work = [
        pltpu.VMEM((2,) + wide, F32),
        pltpu.VMEM((2,) + wide, F32),
        pltpu.VMEM((2,) + wide, F32),
        pltpu.VMEM((2, 2, 2 * size, 2 * size), BF16),
    ]
    better, square = pl.pallas_call(
        side_kernel,
        out_shape=(array(2, *wide), array(2, *wide)),
        in_specs=[VM],
        out_specs=(VM, VM),
        scratch_shapes=work,
        name="side",
        compiler_params=PARAMS,
        cost_estimate=pl.CostEstimate(flops=2 * 10**9, bytes_accessed=2**20, transcendentals=0),
    )(gathered)
    direct = ways_energy <= MOST_STEPS
    pieces = ways_energy if direct else 1
    chunk = size // pieces
    parts = pl.pallas_call(
        functools.partial(green_kernel, pieces),
        out_shape=(array(2, chunk, size),) * pieces,
        in_specs=[VM] * 5,
        out_specs=(VM,) * pieces,
        scratch_shapes=work + [pltpu.VMEM((6, size, size), F32), pltpu.VMEM((2,) + wide, F32), pltpu.VMEM((3,) + wide, F32)],
        name="green",
        compiler_params=PARAMS,
    )(gathered, shares, partner, better, square)
    if not direct:
        green = parts[0].reshape(2, 1, 1, size, size)
        spread = lax.all_to_all(
            parts[0].reshape(2, groups, rows, size).transpose(1, 0, 2, 3),
            ("energy", "role"), split_axis=0, concat_axis=0, tiled=True,
        )
        screened = pl.pallas_call(
            screen_kernel,
            out_shape=array(*spread.shape),
            in_specs=[SM, VM, VM],
            out_specs=VM,
            name="screen",
        )(offsets, weight, spread)
        returned = lax.all_to_all(
            screened, ("energy", "role"), split_axis=0, concat_axis=0, tiled=True
        )
        return green, returned.transpose(1, 0, 2, 3).reshape(2, 1, 1, size, size)

    def join(name, values):
        return pl.pallas_call(
            join_kernel,
            out_shape=array(2, 1, 1, size, size),
            in_specs=[VM] * pieces,
            out_specs=HB,
            scratch_shapes=[pltpu.SemaphoreType.DMA((pieces,))],
            name=name,
            compiler_params=PARAMS,
        )(*values[::-1])

    arrived = exchange(parts)
    green = join("green_out", parts)
    own = pl.pallas_call(
        merge_kernel,
        out_shape=array(2 * chunk * pieces + rows, size),
        in_specs=[VM] * (pieces + 1),
        out_specs=VM,
        name="merge",
        compiler_params=PARAMS,
    )(weight, *arrived[::-1])
    other = swap(own, "role", 1)
    factor = 6.0 / groups / (2.0 * 3.141592653589793) / offsets.shape[0]
    hits = jnp.sum(offsets[None, :] == jnp.arange(groups)[:, None], axis=1, keepdims=True)
    hits = jnp.broadcast_to(factor * hits.astype(F32), (groups, size))
    screened = pl.pallas_call(
        pair_screen_kernel,
        out_shape=(array(2, chunk, size),) * pieces,
        in_specs=[VM, VM, VM],
        out_specs=(VM,) * pieces,
        scratch_shapes=[
            pltpu.VMEM((2 * groups, 2, chunk, size), F32),
            pltpu.VMEM((chunk, size), F32),
        ],
        name="screen",
        compiler_params=PARAMS,
    )(hits, own, other)
    return green, join("sigma_out", exchange(screened))


def solution(mesh):
    in_specs = (
        P(None, ("energy", "role"), "block", None, None),
        P("block", None, None),
        P("block", None, None),
        P("block", ("energy", "role")),
        P(None, "block", None, None),
        P(),
    )
    out_specs = (
        P(None, ("energy", "role"), "block", None, None),
        P(None, ("energy", "role"), "block", None, None),
    )
    return jax.shard_map(body, mesh=mesh, in_specs=in_specs, out_specs=out_specs, check_vma=False)
```

```python
import functools

import jax
import jax.numpy as jnp
from jax import lax
from jax.experimental import pallas as pl
from jax.experimental.pallas import tpu as pltpu
from jax.sharding import PartitionSpec as P

ETA = 0.1
CONTACT = 0.5
F32 = jnp.float32
BF16 = jnp.bfloat16

LOW = 2.5e-4
HEAD = 1.6
STEPS = 7
TRUST = 2e-4
TOL = 1e-6
MAX_SAFE = 300


def step_table(low, steps):
    rows = []
    for _ in range(steps):
        scale = 4.0 / (1.0 + low) ** 2
        rows.append((scale * (1.0 + low), scale))
        low = scale * low
    return rows, 2.0 / (1.0 + low)


def split(value):
    high = value.astype(BF16)
    return high, (value - high.astype(F32)).astype(BF16)


def dot(left, right):
    return jnp.dot(left, right, preferred_element_type=F32)


def dot_turned(left, right):
    return lax.dot_general(left, right, (((1,), (1,)), ((), ())), preferred_element_type=F32)


def normal_matrix(parts, weights):
    return dot_turned(parts[0], weights[0]) + (
        dot_turned(parts[0], weights[1]) + dot_turned(parts[1], weights[0])
    )


def dot3(left, right):
    rows = left[0].shape[0]
    both = dot(jnp.concatenate([left[0], left[1]], axis=0), right[0])
    return (both[:rows] + both[rows:]) + dot(left[0], right[1])


def embed(wide):
    half = wide.shape[1] // 2
    return jnp.concatenate(
        [wide, jnp.concatenate([-wide[:, half:], wide[:, :half]], axis=1)], axis=0
    )


def embed_both(parts):
    return embed(parts[0]), embed(parts[1])


def wide_eye(size):
    row = lax.broadcasted_iota(jnp.int32, (size, 2 * size), 0)
    col = lax.broadcasted_iota(jnp.int32, (size, 2 * size), 1)
    return jnp.where(row == col, 1.0, 0.0).astype(F32)


def adjoint(wide):
    half = wide.shape[1] // 2
    return jnp.concatenate([wide[:, :half].T, -wide[:, half:].T], axis=1)


def rough_inverse(slots, s_ref, x_ref, t_ref, e_ref, beside=()):
    beside = list(beside)
    size = s_ref.shape[1]
    table, last = step_table(LOW, STEPS)
    for slot in slots:
        value = s_ref[slot]
        parts = split(value)
        weights = embed_both(parts)
        e_ref[slot, 0], e_ref[slot, 1] = weights
        t_ref[slot] = normal_matrix(parts, weights)
        x_ref[slot] = adjoint(value)
    for index in range(STEPS):
        lift, scale = table[index]
        for slot in slots:
            power = t_ref[slot]
            approx = x_ref[slot]
            parts = split(power)
            weights = embed_both(parts)
            if index == 0:
                alpha = HEAD * inverse_bound(power)
                t_ref[slot] = (lift * alpha) * power - (scale * alpha * alpha) * dot3(parts, weights)
                x_ref[slot] = (lift * alpha) * approx - (scale * alpha * alpha) * dot3(
                    split(approx), weights
                )
            elif index < STEPS - 1:
                t_ref[slot] = lift * power - scale * dot3(parts, weights)
                x_ref[slot] = lift * approx - scale * dot3(split(approx), weights)
            else:
                x_ref[slot] = (last * lift) * approx - (last * scale) * dot(
                    approx.astype(BF16), weights[0]
                )
        if beside:
            beside.pop(0)()
    assert not beside


def inverse_bound(normal):
    size = normal.shape[0]
    sizes = jnp.sqrt(normal[:, :size] ** 2 + normal[:, size:] ** 2)
    bound = jnp.max(jnp.sum(sizes, axis=0, keepdims=True), axis=1, keepdims=True)
    return jnp.broadcast_to(1.0 / bound, (1, 2 * size))


def correction(slot, x_ref, e_ref):
    approx = x_ref[slot]
    parts = split(approx)
    rest = wide_eye(approx.shape[0]) - dot3(parts, (e_ref[slot, 0], e_ref[slot, 1]))
    rest_parts = split(rest)
    square = dot(rest_parts[0], embed(rest_parts[0]))
    better = approx + dot3(rest_parts, embed_both(parts))
    return better, square


def small(square):
    return jnp.sum(square * square) < TRUST


def safe_inverse(slot, s_ref, x_ref, e_ref):
    value = s_ref[slot]
    parts = split(value)
    weights = embed_both(parts)
    e_ref[slot, 0], e_ref[slot, 1] = weights
    x_ref[slot] = adjoint(value) * inverse_bound(normal_matrix(parts, weights))

    def unfinished(state):
        return jnp.logical_and(state[0] < MAX_SAFE, jnp.logical_not(state[1] < TOL))

    def refine(state):
        approx = x_ref[slot]
        parts = split(approx)
        rest = wide_eye(approx.shape[0]) - dot3(parts, (e_ref[slot, 0], e_ref[slot, 1]))
        x_ref[slot] = approx + dot3(split(rest), embed_both(parts))
        return state[0] + 1, jnp.sum(rest * rest)

    lax.while_loop(unfinished, refine, (jnp.int32(0), jnp.float32(1e30)))


def stack_parts(wide):
    half = wide.shape[1] // 2
    return jnp.concatenate([wide[:, :half], wide[:, half:]], axis=0)


def right_real(wide, matrix):
    rows = wide.shape[0]
    result = dot3(split(stack_parts(wide)), split(matrix))
    return jnp.concatenate([result[:rows], result[rows:]], axis=1)


def fetch(pairs, sems):
    copies = [pltpu.make_async_copy(source, target, sems.at[i]) for i, (source, target) in enumerate(pairs)]
    for copy in copies:
        copy.start()
    return copies


def tile_lines(pattern_ref, which, tile_row, size):
    tiles = pattern_ref.shape[-1]
    lane = lax.broadcasted_iota(jnp.int32, (1, size), 1) // (size // tiles)
    line = jnp.zeros((1, size), F32)
    for column in range(tiles):
        line = jnp.where(lane == column, pattern_ref[which, 0, tile_row, column].astype(F32), line)
    return line


def prepare_kernel(
    total, last_block, pattern_hbm, sigma_hbm, ham_hbm, coupling_hbm,
    out_ref, pattern_ref, sigma_ref, ham_ref, coupling_ref, sems,
):
    size = ham_ref.shape[-1]
    tiles = pattern_ref.shape[-1]
    tile = size // tiles
    copies = fetch(
        (
            (pattern_hbm, pattern_ref),
            (ham_hbm.at[0], ham_ref),
            (coupling_hbm.at[0], coupling_ref),
            (sigma_hbm.at[:, 0, 0], sigma_ref),
        ),
        sems,
    )
    block = lax.axis_index("block")
    role = lax.axis_index("role")
    place = lax.axis_index("energy") * lax.axis_size("role") + role
    row = lax.broadcasted_iota(jnp.int32, (size, size), 0)
    col = lax.broadcasted_iota(jnp.int32, (size, size), 1)
    number = jnp.full((size, size), place, jnp.int32).astype(F32)
    energy = jnp.where(row == col, -3.0 + 6.0 * number / total, 0.0)
    for copy in copies:
        copy.wait()
    mask = jnp.concatenate(
        [jnp.broadcast_to(tile_lines(pattern_ref, 0, t, size), (tile, size)) for t in range(tiles)],
        axis=0,
    )
    masked = ham_ref[...] * mask
    onsite = 0.5 * (masked + masked.T)
    out_ref[:size] = energy - onsite - sigma_ref[0]
    out_ref[size : 2 * size] = jnp.where(row == col, ETA, 0.0) - sigma_ref[1]
    share = out_ref.shape[0] - 2 * size
    out_ref[2 * size :] = coupling_ref[pl.ds(pl.multiple_of(role * share, share), share)]

    @pl.when(block == last_block)
    def _():
        square = dot3(split(coupling_ref[...].T), split(coupling_ref[...]))
        out_ref[size : 2 * size] += CONTACT * square


def weight_kernel(pattern_ref, coulomb_ref, weight_ref):
    rows, size = coulomb_ref.shape
    tile = size // pattern_ref.shape[-1]
    place = lax.axis_index("energy") * lax.axis_size("role") + lax.axis_index("role")
    for local_row in range(rows):
        line = tile_lines(pattern_ref, 1, (place * rows + local_row) // tile, size)
        value = coulomb_ref[local_row : local_row + 1] * line
        weight_ref[local_row : local_row + 1] = value * value


def share_kernel(all_ref, out_ref):
    first = all_ref.shape[1] - out_ref.shape[1]
    for block in range(out_ref.shape[0]):
        out_ref[block] = all_ref[block, first:]


def neighbours():
    own = lax.axis_index("block")
    low_half = own % 2 == 0
    return own, own ^ 2, jnp.where(low_half, 1, 2), jnp.where(low_half, 3, 0)


def wide_base(all_ref, block):
    size = all_ref.shape[-1]
    return jnp.concatenate([all_ref[block, :size], all_ref[block, size : 2 * size]], axis=1)


def side_kernel(all_ref, better_ref, square_ref, s_ref, x_ref, t_ref, e_ref):
    _, _, middle, other = neighbours()
    s_ref[0] = wide_base(all_ref, middle)
    s_ref[1] = wide_base(all_ref, other)
    rough_inverse((0, 1), s_ref, x_ref, t_ref, e_ref)
    for slot in range(2):
        better_ref[slot], square_ref[slot] = correction(slot, x_ref, e_ref)


def green_kernel(pieces, all_ref, mine_ref, theirs_ref, better_ref, square_ref, *refs):
    out_refs, (s_ref, x_ref, t_ref, e_ref, k_ref, up_ref, r_ref) = refs[:-7], refs[-7:]
    size = all_ref.shape[-1]
    own, far, middle, other = neighbours()
    role = lax.axis_index("role")

    def base(block):
        return wide_base(all_ref, block)

    share = mine_ref.shape[1]
    for block in range(3):
        for index, ref in ((role, mine_ref), (1 - role, theirs_ref)):
            k_ref[block, pl.ds(pl.multiple_of(index * share, share), share)] = ref[block]
        k_ref[3 + block] = k_ref[block].T

    def link(source, target):
        return k_ref[jnp.where(target > source, source, 3 + target)]

    beside = jnp.where(own % 2 == 0, 2, 1)
    beside_far = beside == far

    def reduce(better, square):
        def left(matrix, slot):
            first = dot(matrix.astype(BF16), square[slot].astype(BF16))
            return jnp.concatenate([matrix + first[:, :size], first[:, size:]], axis=1)

        def product(first, second):
            return dot3(split(first), embed_both(split(second)))

        far_left = left(link(far, middle), 0)
        far_right = right_real(better[0], link(middle, far))
        side = product(left(link(beside, other), 1), right_real(better[1], link(other, beside)))
        s_ref[0] = base(far) - product(far_left, far_right) - jnp.where(beside_far, side, 0.0)
        s_ref[1] = base(own) - jnp.where(beside_far, 0.0, side)
        up_ref[0] = far_left
        up_ref[1] = far_right

        def prepare_own():
            r_ref[0] = left(link(own, middle), 0)
            r_ref[1] = right_real(better[0], link(middle, own))

        def own_system():
            s_ref[1] -= product(r_ref[0], r_ref[1])

        def coupling_up():
            r_ref[2] = product(r_ref[0], up_ref[1])

        def coupling_down():
            up_ref[1] = product(up_ref[0], r_ref[1])
            up_ref[0] = r_ref[2]

        return prepare_own, own_system, coupling_up, coupling_down

    work = reduce((better_ref[0], better_ref[1]), (square_ref[0], square_ref[1]))
    good = jnp.logical_and(small(square_ref[0]), small(square_ref[1]))

    rough_inverse((0,), s_ref, x_ref, t_ref, e_ref, work)
    better, square = correction(0, x_ref, e_ref)
    good = jnp.logical_and(good, small(square))
    up = up_ref[0]
    left = up + dot(up.astype(BF16), embed(square.astype(BF16)))
    right = dot3(split(better), embed_both(split(up_ref[1])))
    s_ref[0] = s_ref[1] - dot3(split(left), embed_both(split(right)))

    rough_inverse((0,), s_ref, x_ref, t_ref, e_ref)
    better, square = correction(0, x_ref, e_ref)
    good = jnp.logical_and(good, small(square))
    x_ref[0] = better + dot(square.astype(BF16), embed(better.astype(BF16)))

    @pl.when(jnp.logical_not(good))
    def _():
        s_ref[0] = base(middle)
        safe_inverse(0, s_ref, x_ref, e_ref)
        s_ref[1] = base(other)
        safe_inverse(1, s_ref, x_ref, e_ref)
        zero = jnp.zeros((size, 2 * size), F32)
        for step in reduce((x_ref[0], x_ref[1]), (zero, zero)):
            step()
        safe_inverse(0, s_ref, x_ref, e_ref)
        first = dot3(split(up_ref[0]), embed_both(split(x_ref[0])))
        s_ref[0] = s_ref[1] - dot3(split(first), embed_both(split(up_ref[1])))
        safe_inverse(0, s_ref, x_ref, e_ref)

    if pieces == 1:
        out_refs[0][0] = x_ref[0, :, :size]
        out_refs[0][1] = x_ref[0, :, size:]
        return
    rows = size // pieces
    here = lax.axis_index("energy")
    for step in range(pieces):
        part = pl.ds(pl.multiple_of((here ^ step) * rows, rows), rows)
        out_refs[step][0] = x_ref[0, part, :size]
        out_refs[step][1] = x_ref[0, part, size:]


def join_kernel(*refs):
    out_hbm, sems = refs[-2:]
    pieces = len(refs) - 2
    rows = refs[0].shape[1]
    here = lax.axis_index("energy")
    copies = fetch(
        [
            (refs[order(pieces).index(step)], out_hbm.at[:, 0, 0, pl.ds(pl.multiple_of((here ^ step) * rows, rows), rows)])
            for step in range(pieces)
        ],
        sems,
    )
    for copy in copies:
        copy.wait()


def merge_kernel(weight_ref, *refs):
    out_ref = refs[-1]
    rows = refs[0].shape[1]
    for step, ref in zip(order(len(refs) - 1), refs[:-1]):
        for part in range(2):
            start = (2 * step + part) * rows
            out_ref[start : start + rows] = ref[part]
    start = 2 * rows * (len(refs) - 1)
    out_ref[start : start + weight_ref.shape[0]] = weight_ref[...]


def pair_screen_kernel(hits_ref, own_ref, other_ref, *refs):
    out_refs, (g_ref, w_ref) = refs[:-2], refs[-2:]
    pieces = len(out_refs)
    energies = g_ref.shape[0] // 2
    rows = g_ref.shape[2]
    ways = energies // pieces
    here = lax.axis_index("energy")
    role = lax.axis_index("role")
    g_ref[:energies] = jnp.zeros((energies, 2) + g_ref.shape[2:], F32)
    half = w_ref.shape[0] // ways
    start = 2 * rows * pieces
    for index, ref in ((role, own_ref), (1 - role, other_ref)):
        for step in range(pieces):
            n = energies + ways * (here ^ step) + (index if step == 0 else 1 - index)
            for part in range(2):
                first = (2 * step + part) * rows
                g_ref[n, part] = ref[first : first + rows]
        w_ref[pl.ds(pl.multiple_of(index * half, half), half)] = ref[start : start + half]
    totals = [[jnp.zeros(g_ref.shape[2:], F32) for _ in range(2)] for _ in range(pieces)]
    for d in range(energies):
        p_real = jnp.zeros(g_ref.shape[2:], F32)
        p_imag = jnp.zeros(g_ref.shape[2:], F32)
        for n in range(d, energies):
            a, b = g_ref[energies + n, 0], g_ref[energies + n, 1]
            c, e = g_ref[energies + n - d, 0], g_ref[energies + n - d, 1]
            p_real += a * c - b * e
            p_imag += a * e + b * c
        scale = hits_ref[d : d + 1]
        p_real *= scale
        p_imag *= scale
        for step in range(pieces):
            n = energies + ways * (here ^ step) + (role if step == 0 else 1 - role) - d
            a, b = g_ref[n, 0], g_ref[n, 1]
            totals[step][0] += a * p_real - b * p_imag
            totals[step][1] += a * p_imag + b * p_real
    weight = w_ref[...]
    for step in range(pieces):
        out_refs[step][0] = totals[step][0] * weight
        out_refs[step][1] = totals[step][1] * weight


def screen_kernel(offsets_ref, weight_ref, g_ref, out_ref):
    energies = g_ref.shape[0]
    count = offsets_ref.shape[0]
    factor = 6.0 / energies / (2.0 * 3.141592653589793) / count
    weight = weight_ref[...]

    def uses(offset):
        return lax.fori_loop(
            0, count, lambda i, total: total + jnp.where(offsets_ref[i] == offset, 1, 0), jnp.int32(0)
        )

    out_ref[...] = jnp.zeros_like(out_ref)

    @pl.loop(0, energies)
    def _(d):
        hits = uses(d)

        @pl.when(hits > 0)
        def _():
            scale = weight * (factor * hits.astype(F32))

            def gather(n, total):
                a, b, c, e = g_ref[n, 0], g_ref[n, 1], g_ref[n - d, 0], g_ref[n - d, 1]
                return total[0] + a * c - b * e, total[1] + a * e + b * c

            zero = jnp.zeros_like(weight)
            p_real, p_imag = lax.fori_loop(d, energies, gather, (zero, zero))
            p_real, p_imag = p_real * scale, p_imag * scale

            @pl.loop(d, energies)
            def _(n):
                a, b = g_ref[n - d, 0], g_ref[n - d, 1]
                out_ref[n, 0] += a * p_real - b * p_imag
                out_ref[n, 1] += a * p_imag + b * p_real


VM = pl.BlockSpec(memory_space=pltpu.VMEM)
SM = pl.BlockSpec(memory_space=pltpu.SMEM)
HB = pl.BlockSpec(memory_space=pltpu.HBM)
LIMIT = 8 * 2**20
PARAMS = pltpu.CompilerParams(vmem_limit_bytes=LIMIT)
MOST_STEPS = 8


def order(pieces):
    first = [2, 3] if pieces > 3 else []
    return first + [step for step in reversed(range(pieces)) if step not in first]


def array(*shape):
    return jax.ShapeDtypeStruct(shape, F32)


def swap(value, axis, step):
    ways = lax.axis_size(axis)
    return lax.ppermute(value, axis, [(i, i ^ step) for i in range(ways)])


def exchange(values):
    ways, roles = lax.axis_size("energy"), lax.axis_size("role")
    result = list(values)
    for step in reversed(range(1, len(values))):
        pairs = [(i * roles + j, (i ^ step) * roles + 1 - j) for i in range(ways) for j in range(roles)]
        result[step] = lax.ppermute(values[step], ("energy", "role"), pairs)
    return result


def body(sigma_in, hamiltonian, coupling, coulomb, pattern, offsets):
    size = hamiltonian.shape[-1]
    blocks = lax.axis_size("block")
    ways_energy = lax.axis_size("energy")
    ways_role = lax.axis_size("role")
    groups = ways_energy * ways_role
    rows = size // groups
    assert blocks == 4 and sigma_in.shape[1] == 1 and ways_role == 2
    share = size // ways_role
    packed = pl.pallas_call(
        functools.partial(prepare_kernel, groups, blocks - 1),
        out_shape=array(2 * size + share, size),
        in_specs=[HB] * 4,
        out_specs=VM,
        scratch_shapes=[
            pltpu.SMEM(pattern.shape, jnp.int32),
            pltpu.VMEM((2, size, size), F32),
            pltpu.VMEM((size, size), F32),
            pltpu.VMEM((size, size), F32),
            pltpu.SemaphoreType.DMA((4,)),
        ],
        name="prepare",
        compiler_params=PARAMS,
    )(*(pltpu.with_memory_space_constraint(v, pltpu.HBM) for v in (pattern, sigma_in, hamiltonian, coupling)))
    weight = pl.pallas_call(
        weight_kernel,
        out_shape=array(rows, size),
        in_specs=[SM, VM],
        out_specs=VM,
        name="weight",
        compiler_params=PARAMS,
    )(pattern, coulomb.reshape(rows, size))
    gathered = lax.all_gather(packed, "block", axis=0, tiled=False)
    shares = pl.pallas_call(
        share_kernel,
        out_shape=array(blocks - 1, share, size),
        in_specs=[VM],
        out_specs=VM,
        name="share",
        compiler_params=PARAMS,
    )(gathered)
    partner = swap(shares, "role", 1)
    wide = (size, 2 * size)
    work = [
        pltpu.VMEM((2,) + wide, F32),
        pltpu.VMEM((2,) + wide, F32),
        pltpu.VMEM((2,) + wide, F32),
        pltpu.VMEM((2, 2, 2 * size, 2 * size), BF16),
    ]
    better, square = pl.pallas_call(
        side_kernel,
        out_shape=(array(2, *wide), array(2, *wide)),
        in_specs=[VM],
        out_specs=(VM, VM),
        scratch_shapes=work,
        name="side",
        compiler_params=PARAMS,
        cost_estimate=pl.CostEstimate(flops=2 * 10**9, bytes_accessed=2**20, transcendentals=0),
    )(gathered)
    direct = ways_energy <= MOST_STEPS
    pieces = ways_energy if direct else 1
    chunk = size // pieces
    parts = pl.pallas_call(
        functools.partial(green_kernel, pieces),
        out_shape=(array(2, chunk, size),) * pieces,
        in_specs=[VM] * 5,
        out_specs=(VM,) * pieces,
        scratch_shapes=work + [pltpu.VMEM((6, size, size), F32), pltpu.VMEM((2,) + wide, F32), pltpu.VMEM((3,) + wide, F32)],
        name="green",
        compiler_params=PARAMS,
    )(gathered, shares, partner, better, square)
    if not direct:
        green = parts[0].reshape(2, 1, 1, size, size)
        spread = lax.all_to_all(
            parts[0].reshape(2, groups, rows, size).transpose(1, 0, 2, 3),
            ("energy", "role"), split_axis=0, concat_axis=0, tiled=True,
        )
        screened = pl.pallas_call(
            screen_kernel,
            out_shape=array(*spread.shape),
            in_specs=[SM, VM, VM],
            out_specs=VM,
            name="screen",
        )(offsets, weight, spread)
        returned = lax.all_to_all(
            screened, ("energy", "role"), split_axis=0, concat_axis=0, tiled=True
        )
        return green, returned.transpose(1, 0, 2, 3).reshape(2, 1, 1, size, size)

    def join(name, values):
        return pl.pallas_call(
            join_kernel,
            out_shape=array(2, 1, 1, size, size),
            in_specs=[VM] * pieces,
            out_specs=HB,
            scratch_shapes=[pltpu.SemaphoreType.DMA((pieces,))],
            name=name,
            compiler_params=PARAMS,
        )(*(values[i] for i in order(pieces)))

    arrived = exchange(parts)
    green = join("green_out", parts)
    own = pl.pallas_call(
        merge_kernel,
        out_shape=array(2 * chunk * pieces + rows, size),
        in_specs=[VM] * (pieces + 1),
        out_specs=VM,
        name="merge",
        compiler_params=PARAMS,
    )(weight, *(arrived[i] for i in order(pieces)))
    other = swap(own, "role", 1)
    factor = 6.0 / groups / (2.0 * 3.141592653589793) / offsets.shape[0]
    hits = jnp.sum(offsets[None, :] == jnp.arange(groups)[:, None], axis=1, keepdims=True)
    hits = jnp.broadcast_to(factor * hits.astype(F32), (groups, size))
    screened = pl.pallas_call(
        pair_screen_kernel,
        out_shape=(array(2, chunk, size),) * pieces,
        in_specs=[VM, VM, VM],
        out_specs=(VM,) * pieces,
        scratch_shapes=[
            pltpu.VMEM((2 * groups, 2, chunk, size), F32),
            pltpu.VMEM((chunk, size), F32),
        ],
        name="screen",
        compiler_params=PARAMS,
    )(hits, own, other)
    return green, join("sigma_out", exchange(screened))


def solution(mesh):
    in_specs = (
        P(None, ("energy", "role"), "block", None, None),
        P("block", None, None),
        P("block", None, None),
        P("block", ("energy", "role")),
        P(None, "block", None, None),
        P(),
    )
    out_specs = (
        P(None, ("energy", "role"), "block", None, None),
        P(None, ("energy", "role"), "block", None, None),
    )
    return jax.shard_map(body, mesh=mesh, in_specs=in_specs, out_specs=out_specs, check_vma=False)
```

```python
import functools

import jax
import jax.numpy as jnp
from jax import lax
from jax.experimental import pallas as pl
from jax.experimental.pallas import tpu as pltpu
from jax.sharding import PartitionSpec as P

ETA = 0.1
CONTACT = 0.5
F32 = jnp.float32
BF16 = jnp.bfloat16

LOW = 2.5e-4
HEAD = 1.6
STEPS = 7
TRUST = 2e-4
TOL = 1e-6
MAX_SAFE = 300


def step_table(low, steps):
    rows = []
    for _ in range(steps):
        scale = 4.0 / (1.0 + low) ** 2
        rows.append((scale * (1.0 + low), scale))
        low = scale * low
    return rows, 2.0 / (1.0 + low)


def split(value):
    high = value.astype(BF16)
    return high, (value - high.astype(F32)).astype(BF16)


def dot(left, right):
    return jnp.dot(left, right, preferred_element_type=F32)


def dot_turned(left, right):
    return lax.dot_general(left, right, (((1,), (1,)), ((), ())), preferred_element_type=F32)


def normal_matrix(parts, weights):
    return dot_turned(parts[0], weights[0]) + (
        dot_turned(parts[0], weights[1]) + dot_turned(parts[1], weights[0])
    )


def dot3(left, right):
    rows = left[0].shape[0]
    both = dot(jnp.concatenate([left[0], left[1]], axis=0), right[0])
    return (both[:rows] + both[rows:]) + dot(left[0], right[1])


def embed(wide):
    half = wide.shape[1] // 2
    return jnp.concatenate(
        [wide, jnp.concatenate([-wide[:, half:], wide[:, :half]], axis=1)], axis=0
    )


def embed_both(parts):
    return embed(parts[0]), embed(parts[1])


def wide_eye(size):
    row = lax.broadcasted_iota(jnp.int32, (size, 2 * size), 0)
    col = lax.broadcasted_iota(jnp.int32, (size, 2 * size), 1)
    return jnp.where(row == col, 1.0, 0.0).astype(F32)


def adjoint(wide):
    half = wide.shape[1] // 2
    return jnp.concatenate([wide[:, :half].T, -wide[:, half:].T], axis=1)


def rough_inverse(slots, s_ref, x_ref, t_ref, e_ref, beside=()):
    beside = list(beside)
    size = s_ref.shape[1]
    table, last = step_table(LOW, STEPS)
    for slot in slots:
        value = s_ref[slot]
        parts = split(value)
        weights = embed_both(parts)
        e_ref[slot, 0], e_ref[slot, 1] = weights
        t_ref[slot] = normal_matrix(parts, weights)
        x_ref[slot] = adjoint(value)
    for index in range(STEPS):
        lift, scale = table[index]
        for slot in slots:
            power = t_ref[slot]
            approx = x_ref[slot]
            parts = split(power)
            weights = embed_both(parts)
            if index == 0:
                alpha = HEAD * inverse_bound(power)
                t_ref[slot] = (lift * alpha) * power - (scale * alpha * alpha) * dot3(parts, weights)
                x_ref[slot] = (lift * alpha) * approx - (scale * alpha * alpha) * dot3(
                    split(approx), weights
                )
            elif index < STEPS - 1:
                t_ref[slot] = lift * power - scale * dot3(parts, weights)
                x_ref[slot] = lift * approx - scale * dot3(split(approx), weights)
            else:
                x_ref[slot] = (last * lift) * approx - (last * scale) * dot(
                    approx.astype(BF16), weights[0]
                )
        if beside:
            beside.pop(0)()
    assert not beside


def inverse_bound(normal):
    size = normal.shape[0]
    sizes = jnp.sqrt(normal[:, :size] ** 2 + normal[:, size:] ** 2)
    bound = jnp.max(jnp.sum(sizes, axis=0, keepdims=True), axis=1, keepdims=True)
    return jnp.broadcast_to(1.0 / bound, (1, 2 * size))


def correction(slot, x_ref, e_ref):
    approx = x_ref[slot]
    parts = split(approx)
    rest = wide_eye(approx.shape[0]) - dot3(parts, (e_ref[slot, 0], e_ref[slot, 1]))
    rest_parts = split(rest)
    square = dot(rest_parts[0], embed(rest_parts[0]))
    better = approx + dot3(rest_parts, embed_both(parts))
    return better, square


def small(square):
    return jnp.sum(square * square) < TRUST


def safe_inverse(slot, s_ref, x_ref, e_ref):
    value = s_ref[slot]
    parts = split(value)
    weights = embed_both(parts)
    e_ref[slot, 0], e_ref[slot, 1] = weights
    x_ref[slot] = adjoint(value) * inverse_bound(normal_matrix(parts, weights))

    def unfinished(state):
        return jnp.logical_and(state[0] < MAX_SAFE, jnp.logical_not(state[1] < TOL))

    def refine(state):
        approx = x_ref[slot]
        parts = split(approx)
        rest = wide_eye(approx.shape[0]) - dot3(parts, (e_ref[slot, 0], e_ref[slot, 1]))
        x_ref[slot] = approx + dot3(split(rest), embed_both(parts))
        return state[0] + 1, jnp.sum(rest * rest)

    lax.while_loop(unfinished, refine, (jnp.int32(0), jnp.float32(1e30)))


def stack_parts(wide):
    half = wide.shape[1] // 2
    return jnp.concatenate([wide[:, :half], wide[:, half:]], axis=0)


def right_real(wide, matrix):
    rows = wide.shape[0]
    result = dot3(split(stack_parts(wide)), split(matrix))
    return jnp.concatenate([result[:rows], result[rows:]], axis=1)


def fetch(pairs, sems):
    copies = [pltpu.make_async_copy(source, target, sems.at[i]) for i, (source, target) in enumerate(pairs)]
    for copy in copies:
        copy.start()
    return copies


def tile_lines(pattern_ref, which, tile_row, size):
    tiles = pattern_ref.shape[-1]
    lane = lax.broadcasted_iota(jnp.int32, (1, size), 1) // (size // tiles)
    line = jnp.zeros((1, size), F32)
    for column in range(tiles):
        line = jnp.where(lane == column, pattern_ref[which, 0, tile_row, column].astype(F32), line)
    return line


def prepare_kernel(
    total, last_block, pattern_hbm, sigma_hbm, ham_hbm, coupling_hbm,
    out_ref, pattern_ref, sigma_ref, ham_ref, coupling_ref, sems,
):
    size = ham_ref.shape[-1]
    tiles = pattern_ref.shape[-1]
    tile = size // tiles
    copies = fetch(
        (
            (pattern_hbm, pattern_ref),
            (ham_hbm.at[0], ham_ref),
            (coupling_hbm.at[0], coupling_ref),
            (sigma_hbm.at[:, 0, 0], sigma_ref),
        ),
        sems,
    )
    block = lax.axis_index("block")
    role = lax.axis_index("role")
    place = lax.axis_index("energy") * lax.axis_size("role") + role
    row = lax.broadcasted_iota(jnp.int32, (size, size), 0)
    col = lax.broadcasted_iota(jnp.int32, (size, size), 1)
    number = jnp.full((size, size), place, jnp.int32).astype(F32)
    energy = jnp.where(row == col, -3.0 + 6.0 * number / total, 0.0)
    for copy in copies:
        copy.wait()
    mask = jnp.concatenate(
        [jnp.broadcast_to(tile_lines(pattern_ref, 0, t, size), (tile, size)) for t in range(tiles)],
        axis=0,
    )
    masked = ham_ref[...] * mask
    onsite = 0.5 * (masked + masked.T)
    out_ref[:size] = energy - onsite - sigma_ref[0]
    out_ref[size : 2 * size] = jnp.where(row == col, ETA, 0.0) - sigma_ref[1]
    share = out_ref.shape[0] - 2 * size
    out_ref[2 * size :] = coupling_ref[pl.ds(pl.multiple_of(role * share, share), share)]

    @pl.when(block == last_block)
    def _():
        square = dot3(split(coupling_ref[...].T), split(coupling_ref[...]))
        out_ref[size : 2 * size] += CONTACT * square


def weight_kernel(pattern_ref, coulomb_ref, weight_ref):
    rows, size = coulomb_ref.shape
    tile = size // pattern_ref.shape[-1]
    place = lax.axis_index("energy") * lax.axis_size("role") + lax.axis_index("role")
    for local_row in range(rows):
        line = tile_lines(pattern_ref, 1, (place * rows + local_row) // tile, size)
        value = coulomb_ref[local_row : local_row + 1] * line
        weight_ref[local_row : local_row + 1] = value * value


def share_kernel(all_ref, out_ref):
    first = all_ref.shape[1] - out_ref.shape[1]
    for block in range(out_ref.shape[0]):
        out_ref[block] = all_ref[block, first:]


def neighbours():
    own = lax.axis_index("block")
    low_half = own % 2 == 0
    return own, own ^ 2, jnp.where(low_half, 1, 2), jnp.where(low_half, 3, 0)


def wide_base(all_ref, block):
    size = all_ref.shape[-1]
    return jnp.concatenate([all_ref[block, :size], all_ref[block, size : 2 * size]], axis=1)


def side_kernel(all_ref, better_ref, square_ref, s_ref, x_ref, t_ref, e_ref):
    _, _, middle, other = neighbours()
    s_ref[0] = wide_base(all_ref, middle)
    s_ref[1] = wide_base(all_ref, other)
    rough_inverse((0, 1), s_ref, x_ref, t_ref, e_ref)
    for slot in range(2):
        better_ref[slot], square_ref[slot] = correction(slot, x_ref, e_ref)


def green_kernel(pieces, all_ref, mine_ref, theirs_ref, better_ref, square_ref, *refs):
    out_refs, (s_ref, x_ref, t_ref, e_ref, k_ref, up_ref, r_ref) = refs[:-7], refs[-7:]
    size = all_ref.shape[-1]
    own, far, middle, other = neighbours()
    role = lax.axis_index("role")

    def base(block):
        return wide_base(all_ref, block)

    share = mine_ref.shape[1]
    for block in range(3):
        for index, ref in ((role, mine_ref), (1 - role, theirs_ref)):
            k_ref[block, pl.ds(pl.multiple_of(index * share, share), share)] = ref[block]
        k_ref[3 + block] = k_ref[block].T

    def link(source, target):
        return k_ref[jnp.where(target > source, source, 3 + target)]

    beside = jnp.where(own % 2 == 0, 2, 1)
    beside_far = beside == far

    def reduce(better, square):
        def left(matrix, slot):
            first = dot(matrix.astype(BF16), square[slot].astype(BF16))
            return jnp.concatenate([matrix + first[:, :size], first[:, size:]], axis=1)

        def product(first, second):
            return dot3(split(first), embed_both(split(second)))

        far_left = left(link(far, middle), 0)
        far_right = right_real(better[0], link(middle, far))
        side = product(left(link(beside, other), 1), right_real(better[1], link(other, beside)))
        s_ref[0] = base(far) - product(far_left, far_right) - jnp.where(beside_far, side, 0.0)
        s_ref[1] = base(own) - jnp.where(beside_far, 0.0, side)
        up_ref[0] = far_left
        up_ref[1] = far_right

        def prepare_own():
            r_ref[0] = left(link(own, middle), 0)
            r_ref[1] = right_real(better[0], link(middle, own))

        def own_system():
            s_ref[1] -= product(r_ref[0], r_ref[1])

        def coupling_up():
            r_ref[2] = product(r_ref[0], up_ref[1])

        def coupling_down():
            up_ref[1] = product(up_ref[0], r_ref[1])
            up_ref[0] = r_ref[2]

        return prepare_own, own_system, coupling_up, coupling_down

    work = reduce((better_ref[0], better_ref[1]), (square_ref[0], square_ref[1]))
    good = jnp.logical_and(small(square_ref[0]), small(square_ref[1]))

    rough_inverse((0,), s_ref, x_ref, t_ref, e_ref, work)
    better, square = correction(0, x_ref, e_ref)
    good = jnp.logical_and(good, small(square))
    up = up_ref[0]
    left = up + dot(up.astype(BF16), embed(square.astype(BF16)))
    right = dot3(split(better), embed_both(split(up_ref[1])))
    s_ref[0] = s_ref[1] - dot3(split(left), embed_both(split(right)))

    rough_inverse((0,), s_ref, x_ref, t_ref, e_ref)
    better, square = correction(0, x_ref, e_ref)
    good = jnp.logical_and(good, small(square))
    x_ref[0] = better + dot(square.astype(BF16), embed(better.astype(BF16)))

    @pl.when(jnp.logical_not(good))
    def _():
        s_ref[0] = base(middle)
        safe_inverse(0, s_ref, x_ref, e_ref)
        s_ref[1] = base(other)
        safe_inverse(1, s_ref, x_ref, e_ref)
        zero = jnp.zeros((size, 2 * size), F32)
        for step in reduce((x_ref[0], x_ref[1]), (zero, zero)):
            step()
        safe_inverse(0, s_ref, x_ref, e_ref)
        first = dot3(split(up_ref[0]), embed_both(split(x_ref[0])))
        s_ref[0] = s_ref[1] - dot3(split(first), embed_both(split(up_ref[1])))
        safe_inverse(0, s_ref, x_ref, e_ref)

    if pieces == 1:
        out_refs[0][0] = x_ref[0, :, :size]
        out_refs[0][1] = x_ref[0, :, size:]
        return
    rows = size // pieces
    here = lax.axis_index("energy")
    for step in range(pieces):
        part = pl.ds(pl.multiple_of((here ^ step) * rows, rows), rows)
        out_refs[step][0] = x_ref[0, part, :size]
        out_refs[step][1] = x_ref[0, part, size:]


def join_kernel(*refs):
    out_hbm, sems = refs[-2:]
    pieces = len(refs) - 2
    rows = refs[0].shape[1]
    here = lax.axis_index("energy")
    copies = fetch(
        [
            (refs[order(pieces).index(step)], out_hbm.at[:, 0, 0, pl.ds(pl.multiple_of((here ^ step) * rows, rows), rows)])
            for step in range(pieces)
        ],
        sems,
    )
    for copy in copies:
        copy.wait()


def merge_kernel(weight_ref, *refs):
    out_ref = refs[-1]
    rows = refs[0].shape[1]
    for step, ref in zip(order(len(refs) - 1), refs[:-1]):
        for part in range(2):
            start = (2 * step + part) * rows
            out_ref[start : start + rows] = ref[part]
    start = 2 * rows * (len(refs) - 1)
    out_ref[start : start + weight_ref.shape[0]] = weight_ref[...]


def pair_screen_kernel(hits_ref, own_ref, other_ref, *refs):
    out_refs, (g_ref, w_ref) = refs[:-2], refs[-2:]
    pieces = len(out_refs)
    energies = g_ref.shape[0] // 2
    rows = g_ref.shape[2]
    ways = energies // pieces
    here = lax.axis_index("energy")
    role = lax.axis_index("role")
    g_ref[:energies] = jnp.zeros((energies, 2) + g_ref.shape[2:], F32)
    half = w_ref.shape[0] // ways
    start = 2 * rows * pieces
    for index, ref in ((role, own_ref), (1 - role, other_ref)):
        for step in range(pieces):
            n = energies + ways * (here ^ step) + (index if step == 0 else 1 - index)
            for part in range(2):
                first = (2 * step + part) * rows
                g_ref[n, part] = ref[first : first + rows]
        w_ref[pl.ds(pl.multiple_of(index * half, half), half)] = ref[start : start + half]
    totals = [[jnp.zeros(g_ref.shape[2:], F32) for _ in range(2)] for _ in range(pieces)]
    for d in range(energies // 2):
        p_real = jnp.zeros(g_ref.shape[2:], F32)
        p_imag = jnp.zeros(g_ref.shape[2:], F32)
        for n in range(d, energies):
            a, b = g_ref[energies + n, 0], g_ref[energies + n, 1]
            c, e = g_ref[energies + n - d, 0], g_ref[energies + n - d, 1]
            p_real += a * c - b * e
            p_imag += a * e + b * c
        scale = hits_ref[d : d + 1]
        p_real *= scale
        p_imag *= scale
        for step in range(pieces):
            n = energies + ways * (here ^ step) + (role if step == 0 else 1 - role) - d
            a, b = g_ref[n, 0], g_ref[n, 1]
            totals[step][0] += a * p_real - b * p_imag
            totals[step][1] += a * p_imag + b * p_real
    weight = w_ref[...]
    for step in range(pieces):
        out_refs[step][0] = totals[step][0] * weight
        out_refs[step][1] = totals[step][1] * weight


def screen_kernel(offsets_ref, weight_ref, g_ref, out_ref):
    energies = g_ref.shape[0]
    count = offsets_ref.shape[0]
    factor = 6.0 / energies / (2.0 * 3.141592653589793) / count
    weight = weight_ref[...]

    def uses(offset):
        return lax.fori_loop(
            0, count, lambda i, total: total + jnp.where(offsets_ref[i] == offset, 1, 0), jnp.int32(0)
        )

    out_ref[...] = jnp.zeros_like(out_ref)

    @pl.loop(0, energies)
    def _(d):
        hits = uses(d)

        @pl.when(hits > 0)
        def _():
            scale = weight * (factor * hits.astype(F32))

            def gather(n, total):
                a, b, c, e = g_ref[n, 0], g_ref[n, 1], g_ref[n - d, 0], g_ref[n - d, 1]
                return total[0] + a * c - b * e, total[1] + a * e + b * c

            zero = jnp.zeros_like(weight)
            p_real, p_imag = lax.fori_loop(d, energies, gather, (zero, zero))
            p_real, p_imag = p_real * scale, p_imag * scale

            @pl.loop(d, energies)
            def _(n):
                a, b = g_ref[n - d, 0], g_ref[n - d, 1]
                out_ref[n, 0] += a * p_real - b * p_imag
                out_ref[n, 1] += a * p_imag + b * p_real


VM = pl.BlockSpec(memory_space=pltpu.VMEM)
SM = pl.BlockSpec(memory_space=pltpu.SMEM)
HB = pl.BlockSpec(memory_space=pltpu.HBM)
LIMIT = 8 * 2**20
PARAMS = pltpu.CompilerParams(vmem_limit_bytes=LIMIT)
MOST_STEPS = 8


def order(pieces):
    first = [2, 3] if pieces > 3 else []
    return first + [step for step in reversed(range(pieces)) if step not in first]


def array(*shape):
    return jax.ShapeDtypeStruct(shape, F32)


def swap(value, axis, step):
    ways = lax.axis_size(axis)
    return lax.ppermute(value, axis, [(i, i ^ step) for i in range(ways)])


def exchange(values):
    ways, roles = lax.axis_size("energy"), lax.axis_size("role")
    result = list(values)
    for step in reversed(range(1, len(values))):
        pairs = [(i * roles + j, (i ^ step) * roles + 1 - j) for i in range(ways) for j in range(roles)]
        result[step] = lax.ppermute(values[step], ("energy", "role"), pairs)
    return result


def body(sigma_in, hamiltonian, coupling, coulomb, pattern, offsets):
    size = hamiltonian.shape[-1]
    blocks = lax.axis_size("block")
    ways_energy = lax.axis_size("energy")
    ways_role = lax.axis_size("role")
    groups = ways_energy * ways_role
    rows = size // groups
    assert blocks == 4 and sigma_in.shape[1] == 1 and ways_role == 2
    share = size // ways_role
    packed = pl.pallas_call(
        functools.partial(prepare_kernel, groups, blocks - 1),
        out_shape=array(2 * size + share, size),
        in_specs=[HB] * 4,
        out_specs=VM,
        scratch_shapes=[
            pltpu.SMEM(pattern.shape, jnp.int32),
            pltpu.VMEM((2, size, size), F32),
            pltpu.VMEM((size, size), F32),
            pltpu.VMEM((size, size), F32),
            pltpu.SemaphoreType.DMA((4,)),
        ],
        name="prepare",
        compiler_params=PARAMS,
    )(*(pltpu.with_memory_space_constraint(v, pltpu.HBM) for v in (pattern, sigma_in, hamiltonian, coupling)))
    weight = pl.pallas_call(
        weight_kernel,
        out_shape=array(rows, size),
        in_specs=[SM, VM],
        out_specs=VM,
        name="weight",
        compiler_params=PARAMS,
    )(pattern, coulomb.reshape(rows, size))
    gathered = lax.all_gather(packed, "block", axis=0, tiled=False)
    shares = pl.pallas_call(
        share_kernel,
        out_shape=array(blocks - 1, share, size),
        in_specs=[VM],
        out_specs=VM,
        name="share",
        compiler_params=PARAMS,
    )(gathered)
    partner = swap(shares, "role", 1)
    wide = (size, 2 * size)
    work = [
        pltpu.VMEM((2,) + wide, F32),
        pltpu.VMEM((2,) + wide, F32),
        pltpu.VMEM((2,) + wide, F32),
        pltpu.VMEM((2, 2, 2 * size, 2 * size), BF16),
    ]
    better, square = pl.pallas_call(
        side_kernel,
        out_shape=(array(2, *wide), array(2, *wide)),
        in_specs=[VM],
        out_specs=(VM, VM),
        scratch_shapes=work,
        name="side",
        compiler_params=PARAMS,
        cost_estimate=pl.CostEstimate(flops=2 * 10**9, bytes_accessed=2**20, transcendentals=0),
    )(gathered)
    direct = ways_energy <= MOST_STEPS
    pieces = ways_energy if direct else 1
    chunk = size // pieces
    parts = pl.pallas_call(
        functools.partial(green_kernel, pieces),
        out_shape=(array(2, chunk, size),) * pieces,
        in_specs=[VM] * 5,
        out_specs=(VM,) * pieces,
        scratch_shapes=work + [pltpu.VMEM((6, size, size), F32), pltpu.VMEM((2,) + wide, F32), pltpu.VMEM((3,) + wide, F32)],
        name="green",
        compiler_params=PARAMS,
    )(gathered, shares, partner, better, square)
    if not direct:
        green = parts[0].reshape(2, 1, 1, size, size)
        spread = lax.all_to_all(
            parts[0].reshape(2, groups, rows, size).transpose(1, 0, 2, 3),
            ("energy", "role"), split_axis=0, concat_axis=0, tiled=True,
        )
        screened = pl.pallas_call(
            screen_kernel,
            out_shape=array(*spread.shape),
            in_specs=[SM, VM, VM],
            out_specs=VM,
            name="screen",
        )(offsets, weight, spread)
        returned = lax.all_to_all(
            screened, ("energy", "role"), split_axis=0, concat_axis=0, tiled=True
        )
        return green, returned.transpose(1, 0, 2, 3).reshape(2, 1, 1, size, size)

    def join(name, values):
        return pl.pallas_call(
            join_kernel,
            out_shape=array(2, 1, 1, size, size),
            in_specs=[VM] * pieces,
            out_specs=HB,
            scratch_shapes=[pltpu.SemaphoreType.DMA((pieces,))],
            name=name,
            compiler_params=PARAMS,
        )(*(values[i] for i in order(pieces)))

    arrived = exchange(parts)
    green = join("green_out", parts)
    own = pl.pallas_call(
        merge_kernel,
        out_shape=array(2 * chunk * pieces + rows, size),
        in_specs=[VM] * (pieces + 1),
        out_specs=VM,
        name="merge",
        compiler_params=PARAMS,
    )(weight, *(arrived[i] for i in order(pieces)))
    other = swap(own, "role", 1)
    factor = 6.0 / groups / (2.0 * 3.141592653589793) / offsets.shape[0]
    hits = jnp.sum(offsets[None, :] == jnp.arange(groups)[:, None], axis=1, keepdims=True)
    hits = jnp.broadcast_to(factor * hits.astype(F32), (groups, size))
    screened = pl.pallas_call(
        pair_screen_kernel,
        out_shape=(array(2, chunk, size),) * pieces,
        in_specs=[VM, VM, VM],
        out_specs=(VM,) * pieces,
        scratch_shapes=[
            pltpu.VMEM((2 * groups, 2, chunk, size), F32),
            pltpu.VMEM((chunk, size), F32),
        ],
        name="screen",
        compiler_params=PARAMS,
    )(hits, own, other)
    return green, join("sigma_out", exchange(screened))


def solution(mesh):
    in_specs = (
        P(None, ("energy", "role"), "block", None, None),
        P("block", None, None),
        P("block", None, None),
        P("block", ("energy", "role")),
        P(None, "block", None, None),
        P(),
    )
    out_specs = (
        P(None, ("energy", "role"), "block", None, None),
        P(None, ("energy", "role"), "block", None, None),
    )
    return jax.shard_map(body, mesh=mesh, in_specs=in_specs, out_specs=out_specs, check_vma=False)
```
